256 devices in a mesh: wave: 16 (over z, y_hi), lat: 16 (over x, y_lo, core).
Axes of the slice: x: 4, y: 4 (y_hi: 2, y_lo: 2; y = y_hi * 2 + y_lo), z: 8, core: 2. Of those that a mesh axis runs over, the one named last changes fastest.
Arguments:
- control: bfloat16 [640, 640, 256], P('wave', 'lat'), may hold values from -6 to 6
- vert_root: bfloat16 [640, 128, 128], P('wave'), may hold values from -0.5 to 0.5
- legendre: bfloat16 [640, 640, 256], P('lat', 'wave'), may hold values from -0.3125 to 0.3125
- row_wavenumber: int32 [640], P('wave'), may hold values from 0 to 639, each once
- courant_east: float32 [256, 1280, 128], P('wave', 'lat'), may hold values from 0.05 to 0.45
- courant_north: float32 [256, 1280, 128], P('wave', 'lat'), may hold values from 0.05 to 0.45
- east_flags: int32 [256, 1280, 128], P('wave', 'lat'), may hold values 0 or 1
- north_flags: int32 [256, 1280, 128], P('wave', 'lat'), may hold values 0 or 1
Outputs:
- tracer: float32 [256, 1280, 128], P('wave', 'lat')
The draws below stay inside these ranges and needn't reach their ends.
Inputs may be any that keep to these rules, and one draw needn't show every extreme that they name: `row_wavenumber`: A permutation of 0 to 639.
All inputs are finite; a program needn't handle non-finite values. No bound on the sum of `east_flags` or of `north_flags` on one device may be relied on, other than what follows from the above.
Results may differ from the reference program's by a relative error of at most 0.0069.
Values may be sent and summed in bfloat16 or wider, within the bound.
No kernel may reach another device: no remote copies, remote signals or barrier semaphores. Data moves between devices by JAX's collectives and lax.ppermute only.
A program may use at most 64 MiB of HBM per device.

```python
import math
import jax
import jax.numpy as jnp
from jax import lax

NW = 640
LEV = 128
STEPS = 4
LATS = 256
NLON = 1280


def touch_ends(array, key, least, top_value):
    extent = array.shape
    spot = [jax.random.randint(jax.random.fold_in(key, axis), (), 0, extent[axis]) for axis in range(len(extent))]
    array = array.at[tuple(spot)].set(least)
    longest = extent.index(max(extent))
    spot[longest] = (spot[longest] + 1) % extent[longest]
    return array.at[tuple(spot)].set(top_value)


def block_levels(stream_key, dims, split, least, top_value):
    level = 1.0
    for position, parts in split:
        heights = jax.random.uniform(jax.random.fold_in(jax.random.fold_in(stream_key, 6), position), (parts,), jnp.float32, least / len(split), top_value / len(split))
        level = level * jnp.repeat(jnp.exp(heights), dims[position] // parts).reshape((-1,) + (1,) * (len(dims) - 1 - position))
    return level


def normal_values(key, extent, width, bound, pieces=(), kind=jnp.bfloat16):
    entries = jax.random.normal(key, extent, jnp.float32) * width
    if len(pieces) > 0:
        entries = block_levels(key, extent, pieces, -0.22, 0.18) * entries
    return jnp.clip(entries, min=-bound, max=bound).astype(kind)


def setup_inputs(seed: int = 0) -> dict:
    seeds = jax.random.split(jax.random.key(seed), 9)
    return {
        "control": normal_values(seeds[0], (NW, NW, 2 * LEV), 1.0, 6.0, ((0, 16), (1, 16))),
        "vert_root": normal_values(seeds[1], (NW, LEV, LEV), LEV ** -0.5, 0.5, ((0, 16),)),
        "legendre": normal_values(seeds[2], (NW, NW, LATS), (NW // 2) ** -0.5, 0.3125, ((0, 16), (1, 16))),
        "row_wavenumber": jax.random.permutation(seeds[3], NW).astype(jnp.int32),
        "courant_east": jnp.clip(0.05 + 0.39999999 * jax.random.uniform(seeds[4], (LATS, NLON, LEV), jnp.float32) ** block_levels(seeds[4], (LATS, NLON, LEV), ((0, 16), (1, 16)), -0.2, 0.2), 0.05, 0.45),
        "courant_north": jnp.clip(0.05 + 0.39999999 * jax.random.uniform(seeds[5], (LATS, NLON, LEV), jnp.float32) ** block_levels(seeds[5], (LATS, NLON, LEV), ((0, 16), (1, 16)), -0.2, 0.2), 0.05, 0.45),
        "east_flags": touch_ends((jax.random.randint(seeds[6], (LATS, NLON, LEV), 0, 2) < 1).astype(jnp.int32), jax.random.fold_in(seeds[6], 1), 0, 1),
        "north_flags": touch_ends((jax.random.randint(seeds[7], (LATS, NLON, LEV), 0, 2) < 1).astype(jnp.int32), jax.random.fold_in(seeds[7], 1), 0, 1),
    }


def minmod(first_jump, second_jump):
    return jnp.maximum(0.0, jnp.minimum(first_jump, second_jump)) + jnp.minimum(0.0, jnp.maximum(first_jump, second_jump))

def window(values, begin_at, end_at, axis_dim):
    return lax.slice_in_dim(values, begin_at, end_at, axis=axis_dim)

def transport(padded, winds, axis_dim, cell_count):
    jumps = window(padded, 1, cell_count + 4, axis_dim) - window(padded, 0, cell_count + 3, axis_dim)
    limited = minmod(window(jumps, 1, cell_count + 3, axis_dim), window(jumps, 0, cell_count + 2, axis_dim))
    below_cells = window(padded, 1, cell_count + 2, axis_dim)
    above_cells = window(padded, 2, cell_count + 3, axis_dim)
    lower_slope = window(limited, 0, cell_count + 1, axis_dim)
    upper_slope = window(limited, 1, cell_count + 2, axis_dim)
    courant = jnp.abs(winds)
    fluxes = jnp.maximum(winds, 0.0) * (below_cells + 0.5 * (1.0 - courant) * lower_slope) + jnp.minimum(winds, 0.0) * (above_cells - 0.5 * (1.0 - courant) * upper_slope)
    return window(fluxes, 1, cell_count + 1, axis_dim) - window(fluxes, 0, cell_count, axis_dim)

def dft_basis(order_ids, lon_ids, total_lon, total_orders):
    product = order_ids[:, None] * lon_ids[None, :] % total_lon
    phases = product.astype(jnp.float32) * (2.0 * math.pi / total_lon)
    weight = jnp.where(order_ids == 0, 1.0, 2.0).astype(jnp.float32) * (1.0 / math.sqrt(2.0 * total_orders))
    return jnp.stack([weight[:, None] * jnp.cos(phases), -weight[:, None] * jnp.sin(phases)]).astype(jnp.bfloat16)

def reference(control, vert_root, legendre, row_wavenumber, courant_east, courant_north, east_flags, north_flags):
    orders = jnp.arange(NW, dtype=jnp.int32)
    exists = row_wavenumber[:, None] >= orders[None, :]
    spectra = jnp.where(exists[:, :, None], control, jnp.zeros((), control.dtype))
    complex_parts = spectra.reshape(NW, NW, LEV, 2).astype(jnp.float32)
    vertical = jnp.einsum('rmlp,rkl->rmkp', complex_parts, vert_root.astype(jnp.float32)).astype(jnp.bfloat16)
    stacked = vertical.reshape(NW, NW, 2 * LEV)
    modes = jnp.einsum('rmc,mrj->cmj', stacked.astype(jnp.float32), legendre.astype(jnp.float32)).astype(jnp.bfloat16)
    basis = dft_basis(orders, jnp.arange(2 * NW, dtype=jnp.int32), 2 * NW, NW)
    gridded = jnp.einsum('kpmj,pml->jlk', modes.reshape(LEV, 2, NW, LATS).astype(jnp.float32), basis.astype(jnp.float32))
    wind_east = courant_east * (2 * east_flags - 1).astype(jnp.float32)
    wind_north = courant_north * (2 * north_flags - 1).astype(jnp.float32)
    winds_x = jnp.concatenate([wind_east[:, -1:], wind_east], axis=1)
    winds_y = jnp.concatenate([jnp.zeros_like(wind_north[:1]), wind_north], axis=0)
    tracer = gridded
    for repeat in range(STEPS):
        lon_padded = jnp.concatenate([tracer[:, -2:], tracer, tracer[:, :2]], axis=1)
        row_padded = jnp.pad(tracer, ((2, 2), (0, 0), (0, 0)))
        tracer = tracer - transport(lon_padded, winds_x, 1, 2 * NW) - transport(row_padded, winds_y, 0, LATS)
    return tracer
```

```python
import math

import jax
import jax.numpy as jnp
import numpy as np
from jax import lax
from jax.experimental import pallas as pl
from jax.experimental.pallas import tpu as pltpu
from jax.sharding import PartitionSpec as P

NW = 640
LEV = 128
STEPS = 4
NLON = 2 * NW
WAVE = 16
LAT = 16
ROWS = NW // WAVE
ORDERS = NW // LAT
LATS = 256
TILE_R = LATS // WAVE
TILE_X = NLON // LAT
HALO = 2 * STEPS
EXT_X = TILE_X + 2 * HALO
EXT_R = TILE_R + 2 * HALO
PAIRS = 5
SLOTS = 8
GROUP = 5
PAIR_OF = (((0, 0), (0, 1), (1, 0), (1, 1), (2, 0)), ((4, 0), (4, 1), (3, 0), (3, 1), (2, 1)))
ORDER_OF = ((0, 1, 2), (4, 3, 2))
ORDER_SLOT = (0, 0, 1, 1, 2)
R_STEP = 8


def vertical_kernel(info, control, vert, pick, out, scratch):
    step = pl.program_id(0)
    parts = jnp.dot(control[...], pick[...], preferred_element_type=jnp.float32)
    orders = info[ROWS] + lax.broadcasted_iota(jnp.int32, (ORDERS, 2 * LEV), 0)
    for i in range(R_STEP):
        r = step * R_STEP + i
        rows = jnp.where(info[r] >= orders, parts[i * ORDERS : (i + 1) * ORDERS], 0.0)
        both = jnp.concatenate([rows[:, :LEV], rows[:, LEV:]], axis=0).astype(jnp.bfloat16)
        mixed = lax.dot_general(
            both, vert[i], (((1,), (1,)), ((), ())), preferred_element_type=jnp.float32
        )
        for p in range(2):
            scratch[p, pl.ds(r, ORDERS, stride=ROWS), :] = mixed[p * ORDERS : (p + 1) * ORDERS]

    @pl.when(step == pl.num_programs(0) - 1)
    def _():
        for w in range(WAVE):
            for b in range(PAIRS):
                m, p = PAIR_OF[w % 2][b]
                m += GROUP * (w // 2)
                out[w, b] = scratch[p, m * ROWS : (m + 1) * ROWS, :].astype(jnp.bfloat16)


def vertical_parts(control, vert_root, row_wavenumber, first_order):
    info = jnp.concatenate([row_wavenumber, first_order[None]])
    pick = np.zeros((2 * LEV, 2 * LEV), np.float32)
    pick[np.arange(2 * LEV), np.arange(2 * LEV) % 2 * LEV + np.arange(2 * LEV) // 2] = 1.0
    return pl.pallas_call(
        vertical_kernel,
        grid=(ROWS // R_STEP,),
        in_specs=[
            pl.BlockSpec(memory_space=pltpu.SMEM),
            pl.BlockSpec((R_STEP * ORDERS, 2 * LEV), lambda i: (i, 0)),
            pl.BlockSpec((R_STEP, LEV, LEV), lambda i: (i, 0, 0)),
            pl.BlockSpec((2 * LEV, 2 * LEV), lambda i: (0, 0)),
        ],
        out_specs=pl.BlockSpec((WAVE, PAIRS, ROWS, LEV), lambda i: (0, 0, 0, 0)),
        out_shape=jax.ShapeDtypeStruct((WAVE, PAIRS, ROWS, LEV), jnp.bfloat16),
        scratch_shapes=[pltpu.VMEM((2, ORDERS * ROWS, LEV), jnp.float32)],
    )(info, control.reshape(ROWS * ORDERS, 2 * LEV), vert_root, jnp.asarray(pick, jnp.bfloat16))


def modes_kernel(vertical, legendre, out, left, right, result):
    result[...] = jnp.zeros(result.shape, jnp.float32)
    for slot in range(3):
        pairs = [b for b in range(PAIRS) if ORDER_SLOT[b] == slot]
        for s in range(WAVE):
            left[s * ROWS : (s + 1) * ROWS, :] = legendre[s, slot].astype(jnp.float32)
            for i, b in enumerate(pairs):
                right[s * ROWS : (s + 1) * ROWS, i * LEV : (i + 1) * LEV] = vertical[s, b].astype(
                    jnp.float32
                )
        width = len(pairs) * LEV
        total = lax.dot_general(
            left[...].astype(jnp.bfloat16),
            right[:, :width].astype(jnp.bfloat16),
            (((0,), (0,)), ((), ())),
            preferred_element_type=jnp.float32,
        )
        for i, b in enumerate(pairs):
            result[pl.ds(b, LATS, stride=SLOTS), :] = total[:, i * LEV : (i + 1) * LEV]
    out[...] = result[...].astype(jnp.bfloat16)


def modes_of(vertical, legendre):
    return pl.pallas_call(
        modes_kernel,
        out_shape=jax.ShapeDtypeStruct((LATS * SLOTS, LEV), jnp.bfloat16),
        scratch_shapes=[
            pltpu.VMEM((NW, LATS), jnp.float32),
            pltpu.VMEM((NW, 2 * LEV), jnp.float32),
            pltpu.VMEM((LATS * SLOTS, LEV), jnp.float32),
        ],
    )(vertical, legendre)


def fourier_basis():
    order = np.zeros((WAVE, LAT, SLOTS), np.int32)
    part = np.zeros((WAVE, LAT, SLOTS), np.int32)
    used = np.zeros((WAVE, LAT, SLOTS), np.float32)
    for w in range(WAVE):
        for b, (m, p) in enumerate(PAIR_OF[w % 2]):
            order[w, :, b] = np.arange(LAT) * ORDERS + GROUP * (w // 2) + m
            part[w, :, b] = p
            used[w, :, b] = 1.0
    order, part, used = (jnp.asarray(a.reshape(-1)) for a in (order, part, used))
    weight = used * jnp.where(order == 0, 1.0, 2.0).astype(jnp.float32) / math.sqrt(NLON)

    def turn(steps):
        return (steps % NLON).astype(jnp.float32) * (2.0 * math.pi / NLON)

    local = jnp.arange(EXT_X, dtype=jnp.int32) - HALO + NLON
    near = turn(order[None, :] * local[:, None] + part[None, :] * (NLON // 4))
    far = turn(order[None, :] * (TILE_X * jnp.arange(LAT, dtype=jnp.int32))[:, None])
    near_cos, near_sin = weight * jnp.cos(near), weight * jnp.sin(near)
    far_cos, far_sin = jnp.cos(far), jnp.sin(far)
    basis = far_cos[:, None, :] * near_cos[None] - far_sin[:, None, :] * near_sin[None]
    return basis.astype(jnp.bfloat16).reshape(LAT * EXT_X, -1)


def minmod(a, b):
    return jnp.maximum(0.0, jnp.minimum(a, b)) + jnp.minimum(0.0, jnp.maximum(a, b))


def shifted(array, amount):
    return pltpu.roll(array, amount % array.shape[0], 0)


def flux(wind, gain, low, high, low_slope, high_slope):
    forward = wind > 0.0
    return wind * jnp.where(forward, low, high) + gain * jnp.where(forward, low_slope, high_slope)


def advect_kernel(
    where, middle, south, north, ce, cn, ef, nf, west, east, wind_s, wind_n, out, qa, qb, us, gs
):
    band = where[0]
    qa[0:HALO] = south[...].astype(jnp.float32)
    qa[HALO : HALO + TILE_R] = middle[...].astype(jnp.float32)
    qa[HALO + TILE_R :] = north[...].astype(jnp.float32)
    qb[0:HALO] = jnp.zeros((HALO, EXT_X, LEV), jnp.float32)
    qb[HALO + TILE_R :] = jnp.zeros((HALO, EXT_X, LEV), jnp.float32)
    inner = slice(HALO, HALO + TILE_R)
    for d, (size, flag) in enumerate(((ce, ef), (cn, nf))):
        us[d, 0:HALO] = wind_s[d].astype(jnp.float32)
        us[d, HALO + TILE_R :] = wind_n[d].astype(jnp.float32)
        us[d, inner, 0:HALO] = west[d].astype(jnp.float32)
        us[d, inner, HALO + TILE_X :] = east[d].astype(jnp.float32)
        us[d, inner, HALO : HALO + TILE_X] = jnp.where(flag[...] > 0, size[...], -size[...])

    def gains(r, carry):
        for d in range(2):
            speed = jnp.abs(us[d, r])
            gs[d, r] = 0.5 * speed * (1.0 - speed)
        return carry

    lax.fori_loop(0, EXT_R, gains, 0)
    for t in range(1, STEPS + 1):
        old, new = (qa, qb) if t % 2 else (qb, qa)
        low = jnp.where(band == 0, HALO, 2 * t)
        high = jnp.where(band == WAVE - 1, HALO + TILE_R, EXT_R - 2 * t)

        def slope(r):
            here = old[r]
            return minmod(old[r + 1] - here, here - old[r - 1])

        def face(r, low_slope, high_slope):
            return flux(us[1, r], gs[1, r], old[r], old[r + 1], low_slope, high_slope)

        def row(r, carry):
            here_slope, below = carry
            here = old[r]
            next_slope = slope(r + 1)
            above = face(r, here_slope, next_slope)
            right = shifted(here, -1)
            jump = right - here
            steep = minmod(jump, shifted(jump, 1))
            east_face = flux(us[0, r], gs[0, r], here, right, steep, shifted(steep, -1))
            fresh = here - (east_face - shifted(east_face, 1)) - (above - below)
            if t == STEPS:
                out[r - HALO] = fresh[HALO : HALO + TILE_X]
            else:
                new[r] = fresh
            return next_slope, above

        first = slope(low)
        lax.fori_loop(low, high, row, (first, face(low - 1, slope(low - 1), first)))


def advected(band, middle, south, north, winds, halos):
    return pl.pallas_call(
        advect_kernel,
        in_specs=[pl.BlockSpec(memory_space=pltpu.SMEM)]
        + [pl.BlockSpec(memory_space=pltpu.VMEM)] * 11,
        out_shape=jax.ShapeDtypeStruct((TILE_R, TILE_X, LEV), jnp.float32),
        scratch_shapes=[
            pltpu.VMEM((EXT_R, EXT_X, LEV), jnp.float32),
            pltpu.VMEM((EXT_R, EXT_X, LEV), jnp.float32),
            pltpu.VMEM((2, EXT_R, EXT_X, LEV), jnp.float32),
            pltpu.VMEM((2, EXT_R, EXT_X, LEV), jnp.float32),
        ],
    )(band[None], middle, south, north, *winds, *halos)


def from_below(block, axis, wrap):
    pairs = [(i, (i + 1) % 16) for i in range(16 if wrap else 15)]
    return lax.ppermute(block, axis, pairs)


def from_above(block, axis, wrap):
    pairs = [((i + 1) % 16, i) for i in range(16 if wrap else 15)]
    return lax.ppermute(block, axis, pairs)


def per_device(
    control,
    vert_root,
    legendre,
    row_wavenumber,
    courant_east,
    courant_north,
    east_flags,
    north_flags,
):
    lat = lax.axis_index("lat").astype(jnp.int32)
    wave = lax.axis_index("wave").astype(jnp.int32)
    groups = legendre.reshape(WAVE // 2, GROUP, ROWS, LATS)
    legendre_out = jnp.stack(
        [jnp.stack([groups[:, m] for m in orders], axis=1) for orders in ORDER_OF], axis=1
    ).reshape(WAVE, 3, ROWS, LATS)
    legendre_in = lax.all_to_all(legendre_out, "wave", 0, 0, tiled=True)
    vertical_out = vertical_parts(control, vert_root, row_wavenumber, lat * ORDERS)
    vertical_in = lax.all_to_all(vertical_out, "wave", 0, 0, tiled=True)

    winds = jnp.stack(
        [
            jnp.where(flag > 0, size, -size).astype(jnp.bfloat16)
            for size, flag in ((courant_east, east_flags), (courant_north, north_flags))
        ]
    )
    west = from_below(winds[:, :, -HALO:], "lat", True)
    east = from_above(winds[:, :, :HALO], "lat", True)
    wide = jnp.concatenate([west, winds, east], axis=2)

    modes = modes_of(vertical_in, legendre_in).reshape(LATS, SLOTS, LEV)
    modes = lax.all_to_all(modes, ("wave", "lat"), 0, 0, tiled=True)
    wind_s = from_below(wide[:, -HALO:], "wave", False)
    wind_n = from_above(wide[:, :HALO], "wave", False)
    row = jnp.dot(
        fourier_basis(), modes.reshape(LATS * SLOTS, LEV), preferred_element_type=jnp.float32
    ).astype(jnp.bfloat16)
    middle = lax.all_to_all(row.reshape(LAT, EXT_X, LEV), "lat", 0, 0, tiled=True)
    south = from_below(middle[-HALO:], "wave", False)
    north = from_above(middle[:HALO], "wave", False)
    return advected(
        wave,
        middle,
        south,
        north,
        (courant_east, courant_north, east_flags, north_flags),
        (west, east, wind_s, wind_n),
    )


def solution(mesh):
    return jax.shard_map(
        per_device,
        mesh=mesh,
        in_specs=(
            P("wave", "lat", None),
            P("wave", None, None),
            P("lat", "wave", None),
            P("wave"),
            P("wave", "lat", None),
            P("wave", "lat", None),
            P("wave", "lat", None),
            P("wave", "lat", None),
        ),
        out_specs=P("wave", "lat", None),
        check_vma=False,
    )
```

```python
import math

import jax
import jax.numpy as jnp
import numpy as np
from jax import lax
from jax.experimental import pallas as pl
from jax.experimental.pallas import tpu as pltpu
from jax.sharding import PartitionSpec as P

NW = 640
LEV = 128
STEPS = 4
NLON = 2 * NW
WAVE = 16
LAT = 16
ROWS = NW // WAVE
ORDERS = NW // LAT
LATS = 256
TILE_R = LATS // WAVE
TILE_X = NLON // LAT
HALO = 2 * STEPS
EXT_X = TILE_X + 2 * HALO
EXT_R = TILE_R + 2 * HALO
PAIRS = 5
SLOTS = 8
GROUP = 5
PAIR_OF = (((0, 0), (0, 1), (1, 0), (1, 1), (2, 0)), ((4, 0), (4, 1), (3, 0), (3, 1), (2, 1)))
ORDER_SLOT = (0, 0, 1, 1, 2)
R_STEP = 8
BLOCKS = PAIRS + 6
PARAMS = pltpu.CompilerParams(vmem_limit_bytes=24 * 1024 * 1024)


def packing_kernel(wavenumber, first, control, vert, pick, legendre, out, scratch):
    step = pl.program_id(0)
    for i in range(R_STEP):
        m = step * R_STEP + i
        z = m // GROUP
        place = m - GROUP * z
        late = place > 2
        w = 2 * z + jnp.where(late, 1, 0)
        slot = PAIRS + 2 * jnp.where(late, GROUP - 1 - place, place)
        for h in range(2):
            half = legendre[i, :, h * LEV : (h + 1) * LEV]
            out[w, slot + h] = half

            @pl.when(place == 2)
            def _():
                out[w + 1, slot + h] = half

    parts = jnp.dot(control[...], pick[...], preferred_element_type=jnp.float32)
    orders = first[0] + lax.broadcasted_iota(jnp.int32, (ORDERS, 2 * LEV), 0)
    for i in range(R_STEP):
        r = step * R_STEP + i
        rows = jnp.where(wavenumber[r] >= orders, parts[i * ORDERS : (i + 1) * ORDERS], 0.0)
        both = jnp.concatenate([rows[:, :LEV], rows[:, LEV:]], axis=0).astype(jnp.bfloat16)
        mixed = lax.dot_general(
            both, vert[i], (((1,), (1,)), ((), ())), preferred_element_type=jnp.float32
        )
        for p in range(2):
            scratch[p, pl.ds(r, ORDERS, stride=ROWS), :] = mixed[p * ORDERS : (p + 1) * ORDERS]

    @pl.when(step == pl.num_programs(0) - 1)
    def _():
        for w in range(WAVE):
            for b in range(PAIRS):
                m, p = PAIR_OF[w % 2][b]
                m += GROUP * (w // 2)
                out[w, b] = scratch[p, m * ROWS : (m + 1) * ROWS, :].astype(jnp.bfloat16)


def packed_inputs(control, vert_root, legendre, row_wavenumber, first_order):
    pick = np.zeros((2 * LEV, 2 * LEV), np.float32)
    pick[np.arange(2 * LEV), np.arange(2 * LEV) % 2 * LEV + np.arange(2 * LEV) // 2] = 1.0
    return pl.pallas_call(
        packing_kernel,
        grid=(ROWS // R_STEP,),
        in_specs=[
            pl.BlockSpec(memory_space=pltpu.SMEM),
            pl.BlockSpec(memory_space=pltpu.SMEM),
            pl.BlockSpec((R_STEP * ORDERS, 2 * LEV), lambda i: (i, 0)),
            pl.BlockSpec((R_STEP, LEV, LEV), lambda i: (i, 0, 0)),
            pl.BlockSpec((2 * LEV, 2 * LEV), lambda i: (0, 0)),
            pl.BlockSpec((R_STEP, ROWS, LATS), lambda i: (i, 0, 0)),
        ],
        out_specs=pl.BlockSpec((WAVE, BLOCKS, ROWS, LEV), lambda i: (0, 0, 0, 0)),
        out_shape=jax.ShapeDtypeStruct((WAVE, BLOCKS, ROWS, LEV), jnp.bfloat16),
        scratch_shapes=[pltpu.VMEM((2, ORDERS * ROWS, LEV), jnp.float32)],
    )(
        row_wavenumber,
        first_order[None],
        control.reshape(ROWS * ORDERS, 2 * LEV),
        vert_root,
        jnp.asarray(pick, jnp.bfloat16),
        legendre,
    )


def modes_kernel(packed, out, left, right, result):
    result[...] = jnp.zeros(result.shape, jnp.float32)
    for slot in range(3):
        pairs = [b for b in range(PAIRS) if ORDER_SLOT[b] == slot]
        for s in range(WAVE):
            rows = slice(s * ROWS, (s + 1) * ROWS)
            for h in range(2):
                half = packed[s, PAIRS + 2 * slot + h]
                left[rows, h * LEV : (h + 1) * LEV] = half.astype(jnp.float32)
            for i, b in enumerate(pairs):
                right[rows, i * LEV : (i + 1) * LEV] = packed[s, b].astype(jnp.float32)
        width = len(pairs) * LEV
        total = lax.dot_general(
            left[...].astype(jnp.bfloat16),
            right[:, :width].astype(jnp.bfloat16),
            (((0,), (0,)), ((), ())),
            preferred_element_type=jnp.float32,
        )
        for i, b in enumerate(pairs):
            result[pl.ds(b, LATS, stride=SLOTS), :] = total[:, i * LEV : (i + 1) * LEV]
    out[...] = result[...].astype(jnp.bfloat16)


def modes_of(packed):
    return pl.pallas_call(
        modes_kernel,
        out_shape=jax.ShapeDtypeStruct((LATS * SLOTS, LEV), jnp.bfloat16),
        scratch_shapes=[
            pltpu.VMEM((NW, LATS), jnp.float32),
            pltpu.VMEM((NW, 2 * LEV), jnp.float32),
            pltpu.VMEM((LATS * SLOTS, LEV), jnp.float32),
        ],
        compiler_params=PARAMS,
    )(packed)


def angle_tables():
    order = np.zeros((PAIRS, WAVE, LAT), np.int32)
    part = np.zeros((PAIRS, WAVE, LAT), np.int32)
    for w in range(WAVE):
        for b, (m, p) in enumerate(PAIR_OF[w % 2]):
            order[b, w] = np.arange(LAT) * ORDERS + GROUP * (w // 2) + m
            part[b, w] = p
    order, part = (jnp.asarray(a.reshape(-1)) for a in (order, part))
    weight = jnp.where(order == 0, 1.0, 2.0).astype(jnp.float32) * (1.0 / math.sqrt(NLON))

    def turn(steps):
        return (steps % NLON).astype(jnp.float32) * (2.0 * math.pi / NLON)

    local = jnp.arange(EXT_X, dtype=jnp.int32) - HALO + NLON
    near = turn(order[None, :] * local[:, None] + part[None, :] * (NLON // 4))
    far = turn(order[None, :] * (TILE_X * jnp.arange(LAT // 2 + 1, dtype=jnp.int32))[:, None])
    return weight * jnp.cos(near), weight * jnp.sin(near), jnp.cos(far), jnp.sin(far)


def fourier_kernel(modes, near_cos, near_sin, far_cos, far_sin, out, wide, rhs):
    wide[...] = modes[...].astype(jnp.float32)
    for b in range(PAIRS):
        rhs[b * LATS : (b + 1) * LATS] = wide[pl.ds(b, LATS, stride=SLOTS), :].astype(jnp.bfloat16)

    def put(band, basis):
        total = jnp.dot(basis.astype(jnp.bfloat16), rhs[...], preferred_element_type=jnp.float32)
        out[band] = total.astype(jnp.bfloat16)

    for b in range(LAT // 2 + 1):
        even = far_cos[b : b + 1, :] * near_cos[...]
        odd = far_sin[b : b + 1, :] * near_sin[...]
        put(b, even - odd)
        if 0 < b < LAT // 2:
            put(LAT - b, even + odd)


def latitude_row(modes):
    return pl.pallas_call(
        fourier_kernel,
        out_shape=jax.ShapeDtypeStruct((LAT, EXT_X, LEV), jnp.bfloat16),
        scratch_shapes=[
            pltpu.VMEM((LATS * SLOTS, LEV), jnp.float32),
            pltpu.VMEM((LATS * PAIRS, LEV), jnp.bfloat16),
        ],
        compiler_params=PARAMS,
    )(modes, *angle_tables())


def minmod(a, b):
    return jnp.maximum(jnp.minimum(a, b), jnp.minimum(jnp.maximum(a, b), 0.0))


def shifted(array, amount):
    return pltpu.roll(array, amount % array.shape[0], 0)


def flux(wind, gain, low, high, low_slope, high_slope):
    forward = wind > 0.0
    return wind * jnp.where(forward, low, high) + gain * jnp.where(forward, low_slope, high_slope)


def advect_kernel(
    where, middle, south, north, ce, cn, ef, nf, west, east, wind_s, wind_n, out, qa, qb, us, gs
):
    band = where[0]
    qa[0:HALO] = south[...].astype(jnp.float32)
    qa[HALO : HALO + TILE_R] = middle[...].astype(jnp.float32)
    qa[HALO + TILE_R :] = north[...].astype(jnp.float32)
    qb[0:HALO] = jnp.zeros((HALO, EXT_X, LEV), jnp.float32)
    qb[HALO + TILE_R :] = jnp.zeros((HALO, EXT_X, LEV), jnp.float32)
    inner = slice(HALO, HALO + TILE_R)
    for d, (size, flag) in enumerate(((ce, ef), (cn, nf))):
        us[d, 0:HALO] = wind_s[d].astype(jnp.float32)
        us[d, HALO + TILE_R :] = wind_n[d].astype(jnp.float32)
        us[d, inner, 0:HALO] = west[d].astype(jnp.float32)
        us[d, inner, HALO + TILE_X :] = east[d].astype(jnp.float32)
        us[d, inner, HALO : HALO + TILE_X] = jnp.where(flag[...] > 0, size[...], -size[...])

    def gains(r, carry):
        for d in range(2):
            speed = jnp.abs(us[d, r])
            gs[d, r] = 0.5 * speed * (1.0 - speed)
        return carry

    lax.fori_loop(0, EXT_R, gains, 0)
    for t in range(1, STEPS + 1):
        old, new = (qa, qb) if t % 2 else (qb, qa)
        low = jnp.where(band == 0, HALO, 2 * t)
        high = jnp.where(band == WAVE - 1, HALO + TILE_R, EXT_R - 2 * t)

        def slope(r):
            here = old[r]
            return minmod(old[r + 1] - here, here - old[r - 1])

        def face(r, low_slope, high_slope):
            return flux(us[1, r], gs[1, r], old[r], old[r + 1], low_slope, high_slope)

        def row(r, carry):
            here_slope, below = carry
            here = old[r]
            next_slope = slope(r + 1)
            above = face(r, here_slope, next_slope)
            right = shifted(here, -1)
            jump = right - here
            steep = minmod(jump, shifted(jump, 1))
            east_face = flux(us[0, r], gs[0, r], here, right, steep, shifted(steep, -1))
            fresh = here - (east_face - shifted(east_face, 1)) - (above - below)
            if t == STEPS:
                out[r - HALO] = fresh[HALO : HALO + TILE_X]
            else:
                new[r] = fresh
            return next_slope, above

        first = slope(low)
        lax.fori_loop(low, high, row, (first, face(low - 1, slope(low - 1), first)))


def advected(band, middle, south, north, winds, halos):
    return pl.pallas_call(
        advect_kernel,
        in_specs=[pl.BlockSpec(memory_space=pltpu.SMEM)]
        + [pl.BlockSpec(memory_space=pltpu.VMEM)] * 11,
        out_shape=jax.ShapeDtypeStruct((TILE_R, TILE_X, LEV), jnp.float32),
        scratch_shapes=[
            pltpu.VMEM((EXT_R, EXT_X, LEV), jnp.float32),
            pltpu.VMEM((EXT_R, EXT_X, LEV), jnp.float32),
            pltpu.VMEM((2, EXT_R, EXT_X, LEV), jnp.float32),
            pltpu.VMEM((2, EXT_R, EXT_X, LEV), jnp.float32),
        ],
        compiler_params=PARAMS,
    )(band[None], middle, south, north, *winds, *halos)


def from_below(block, axis, wrap):
    pairs = [(i, (i + 1) % 16) for i in range(16 if wrap else 15)]
    return lax.ppermute(block, axis, pairs)


def from_above(block, axis, wrap):
    pairs = [((i + 1) % 16, i) for i in range(16 if wrap else 15)]
    return lax.ppermute(block, axis, pairs)


def per_device(
    control,
    vert_root,
    legendre,
    row_wavenumber,
    courant_east,
    courant_north,
    east_flags,
    north_flags,
):
    lat = lax.axis_index("lat").astype(jnp.int32)
    wave = lax.axis_index("wave").astype(jnp.int32)
    packed = packed_inputs(control, vert_root, legendre, row_wavenumber, lat * ORDERS)
    winds = jnp.stack(
        [
            jnp.where(flag > 0, size, -size).astype(jnp.bfloat16)
            for size, flag in ((courant_east, east_flags), (courant_north, north_flags))
        ]
    )
    west = from_below(winds[:, :, -HALO:], "lat", True)
    east = from_above(winds[:, :, :HALO], "lat", True)
    wide = jnp.concatenate([west, winds, east], axis=2)
    packed = lax.all_to_all(packed, "wave", 0, 0, tiled=True)
    packed, wide = lax.optimization_barrier((packed, wide))
    modes = modes_of(packed)
    modes, wide = lax.optimization_barrier((modes, wide))
    wind_s = from_below(wide[:, -HALO:], "wave", False)
    wind_n = from_above(wide[:, :HALO], "wave", False)
    modes = lax.all_to_all(modes.reshape(LATS, SLOTS, LEV), ("wave", "lat"), 0, 0, tiled=True)
    modes, wind_s, wind_n = lax.optimization_barrier((modes, wind_s, wind_n))
    row = latitude_row(modes.reshape(LATS * SLOTS, LEV))
    middle = lax.all_to_all(row, "lat", 0, 0, tiled=True)
    south = from_below(middle[-HALO:], "wave", False)
    north = from_above(middle[:HALO], "wave", False)
    return advected(
        wave,
        middle,
        south,
        north,
        (courant_east, courant_north, east_flags, north_flags),
        (west, east, wind_s, wind_n),
    )


def solution(mesh):
    return jax.shard_map(
        per_device,
        mesh=mesh,
        in_specs=(
            P("wave", "lat", None),
            P("wave", None, None),
            P("lat", "wave", None),
            P("wave"),
            P("wave", "lat", None),
            P("wave", "lat", None),
            P("wave", "lat", None),
            P("wave", "lat", None),
        ),
        out_specs=P("wave", "lat", None),
        check_vma=False,
    )
```

```python
import math

import jax
import jax.numpy as jnp
import numpy as np
from jax import lax
from jax.experimental import pallas as pl
from jax.experimental.pallas import tpu as pltpu
from jax.sharding import PartitionSpec as P

NW = 640
LEV = 128
STEPS = 4
NLON = 2 * NW
WAVE = 16
LAT = 16
ROWS = NW // WAVE
ORDERS = NW // LAT
LATS = 256
TILE_R = LATS // WAVE
TILE_X = NLON // LAT
HALO = 2 * STEPS
EXT_X = TILE_X + 2 * HALO
EXT_R = TILE_R + 2 * HALO
PAIRS = 5
SLOTS = 8
GROUP = 5
PAIR_OF = (((0, 0), (0, 1), (1, 0), (1, 1), (2, 0)), ((4, 0), (4, 1), (3, 0), (3, 1), (2, 1)))
ORDER_SLOT = (0, 0, 1, 1, 2)
R_STEP = 8
FAR = 16
BLOCKS = PAIRS + 6
PARAMS = pltpu.CompilerParams(vmem_limit_bytes=24 * 1024 * 1024)


def packing_kernel(wavenumber, first, control, vert, pick, legendre, out, scratch):
    step = pl.program_id(0)
    for i in range(R_STEP):
        m = step * R_STEP + i
        z = m // GROUP
        place = m - GROUP * z
        late = place > 2
        w = 2 * z + jnp.where(late, 1, 0)
        slot = PAIRS + 2 * jnp.where(late, GROUP - 1 - place, place)
        for h in range(2):
            half = legendre[i, :, h * LEV : (h + 1) * LEV]
            out[w, slot + h] = half

            @pl.when(place == 2)
            def _():
                out[w + 1, slot + h] = half

    parts = jnp.dot(control[...], pick[...], preferred_element_type=jnp.float32)
    orders = first[0] + lax.broadcasted_iota(jnp.int32, (ORDERS, 2 * LEV), 0)
    for i in range(R_STEP):
        r = step * R_STEP + i
        rows = jnp.where(wavenumber[r] >= orders, parts[i * ORDERS : (i + 1) * ORDERS], 0.0)
        both = jnp.concatenate([rows[:, :LEV], rows[:, LEV:]], axis=0).astype(jnp.bfloat16)
        mixed = lax.dot_general(
            both, vert[i], (((1,), (1,)), ((), ())), preferred_element_type=jnp.float32
        )
        for p in range(2):
            scratch[p, pl.ds(r, ORDERS, stride=ROWS), :] = mixed[p * ORDERS : (p + 1) * ORDERS]

    @pl.when(step == pl.num_programs(0) - 1)
    def _():
        for w in range(WAVE):
            for b in range(PAIRS):
                m, p = PAIR_OF[w % 2][b]
                m += GROUP * (w // 2)
                out[w, b] = scratch[p, m * ROWS : (m + 1) * ROWS, :].astype(jnp.bfloat16)


def packed_inputs(control, vert_root, legendre, row_wavenumber, first_order):
    pick = np.zeros((2 * LEV, 2 * LEV), np.float32)
    pick[np.arange(2 * LEV), np.arange(2 * LEV) % 2 * LEV + np.arange(2 * LEV) // 2] = 1.0
    return pl.pallas_call(
        packing_kernel,
        grid=(ROWS // R_STEP,),
        in_specs=[
            pl.BlockSpec(memory_space=pltpu.SMEM),
            pl.BlockSpec(memory_space=pltpu.SMEM),
            pl.BlockSpec((R_STEP * ORDERS, 2 * LEV), lambda i: (i, 0)),
            pl.BlockSpec((R_STEP, LEV, LEV), lambda i: (i, 0, 0)),
            pl.BlockSpec((2 * LEV, 2 * LEV), lambda i: (0, 0)),
            pl.BlockSpec((R_STEP, ROWS, LATS), lambda i: (i, 0, 0)),
        ],
        out_specs=pl.BlockSpec((WAVE, BLOCKS, ROWS, LEV), lambda i: (0, 0, 0, 0)),
        out_shape=jax.ShapeDtypeStruct((WAVE, BLOCKS, ROWS, LEV), jnp.bfloat16),
        scratch_shapes=[pltpu.VMEM((2, ORDERS * ROWS, LEV), jnp.float32)],
    )(
        row_wavenumber,
        first_order[None],
        control.reshape(ROWS * ORDERS, 2 * LEV),
        vert_root,
        jnp.asarray(pick, jnp.bfloat16),
        legendre,
    )


def modes_kernel(packed, out, left, right, result):
    result[...] = jnp.zeros(result.shape, jnp.float32)
    for slot in range(3):
        pairs = [b for b in range(PAIRS) if ORDER_SLOT[b] == slot]
        for s in range(WAVE):
            rows = slice(s * ROWS, (s + 1) * ROWS)
            for h in range(2):
                half = packed[s, PAIRS + 2 * slot + h]
                left[rows, h * LEV : (h + 1) * LEV] = half.astype(jnp.float32)
            for i, b in enumerate(pairs):
                right[rows, i * LEV : (i + 1) * LEV] = packed[s, b].astype(jnp.float32)
        width = len(pairs) * LEV
        total = lax.dot_general(
            left[...].astype(jnp.bfloat16),
            right[:, :width].astype(jnp.bfloat16),
            (((0,), (0,)), ((), ())),
            preferred_element_type=jnp.float32,
        )
        for i, b in enumerate(pairs):
            result[pl.ds(b, LATS, stride=SLOTS), :] = total[:, i * LEV : (i + 1) * LEV]
    out[...] = result[...].astype(jnp.bfloat16)


def modes_of(packed):
    return pl.pallas_call(
        modes_kernel,
        out_shape=jax.ShapeDtypeStruct((LATS * SLOTS, LEV), jnp.bfloat16),
        scratch_shapes=[
            pltpu.VMEM((NW, LATS), jnp.float32),
            pltpu.VMEM((NW, 2 * LEV), jnp.float32),
            pltpu.VMEM((LATS * SLOTS, LEV), jnp.float32),
        ],
        compiler_params=PARAMS,
    )(packed)


def angle_tables():
    order = np.zeros((PAIRS, WAVE, LAT), np.int32)
    part = np.zeros((PAIRS, WAVE, LAT), np.int32)
    for w in range(WAVE):
        for b, (m, p) in enumerate(PAIR_OF[w % 2]):
            order[b, w] = np.arange(LAT) * ORDERS + GROUP * (w // 2) + m
            part[b, w] = p
    order, part = (jnp.asarray(a.reshape(-1)) for a in (order, part))
    weight = jnp.where(order == 0, 1.0, 2.0).astype(jnp.float32) * (1.0 / math.sqrt(NLON))

    def turn(steps):
        return (steps % NLON).astype(jnp.float32) * (2.0 * math.pi / NLON)

    local = jnp.arange(EXT_X, dtype=jnp.int32) - HALO + NLON
    near = turn(order[None, :] * local[:, None] + part[None, :] * (NLON // 4))
    far = turn(order[None, :] * (TILE_X * jnp.arange(FAR, dtype=jnp.int32))[:, None])
    return jnp.concatenate(
        [weight * jnp.cos(near), weight * jnp.sin(near), jnp.cos(far), jnp.sin(far)]
    )


def fourier_kernel(modes, tables, out, wide, rhs):
    near_cos = tables.at[0:EXT_X]
    near_sin = tables.at[EXT_X : 2 * EXT_X]
    far_cos = tables.at[2 * EXT_X : 2 * EXT_X + FAR]
    far_sin = tables.at[2 * EXT_X + FAR : 2 * EXT_X + 2 * FAR]
    wide[...] = modes[...].astype(jnp.float32)
    for b in range(PAIRS):
        rhs[b * LATS : (b + 1) * LATS] = wide[pl.ds(b, LATS, stride=SLOTS), :].astype(jnp.bfloat16)

    def put(band, basis):
        total = jnp.dot(basis.astype(jnp.bfloat16), rhs[...], preferred_element_type=jnp.float32)
        out[band] = total.astype(jnp.bfloat16)

    for b in range(LAT // 2 + 1):
        even = far_cos[b : b + 1, :] * near_cos[...]
        odd = far_sin[b : b + 1, :] * near_sin[...]
        put(b, even - odd)
        if 0 < b < LAT // 2:
            put(LAT - b, even + odd)


def latitude_row(modes, tables):
    return pl.pallas_call(
        fourier_kernel,
        out_shape=jax.ShapeDtypeStruct((LAT, EXT_X, LEV), jnp.bfloat16),
        scratch_shapes=[
            pltpu.VMEM((LATS * SLOTS, LEV), jnp.float32),
            pltpu.VMEM((LATS * PAIRS, LEV), jnp.bfloat16),
        ],
    )(modes, tables)


def minmod(a, b):
    return jnp.maximum(jnp.minimum(a, b), jnp.minimum(jnp.maximum(a, b), 0.0))


def shifted(array, amount):
    return pltpu.roll(array, amount % array.shape[0], 0)


def flux(wind, gain, low, high, low_slope, high_slope):
    forward = wind > 0.0
    return wind * jnp.where(forward, low, high) + gain * jnp.where(forward, low_slope, high_slope)


def advect_kernel(
    where, middle, halo, ce, cn, ef, nf, west, east, wind_s, wind_n, out, qa, qb, us, gs
):
    band = where[0]
    qa[0:HALO] = halo[HALO:].astype(jnp.float32)
    qa[HALO : HALO + TILE_R] = middle[...].astype(jnp.float32)
    qa[HALO + TILE_R :] = halo[:HALO].astype(jnp.float32)
    qb[0:HALO] = jnp.zeros((HALO, EXT_X, LEV), jnp.float32)
    qb[HALO + TILE_R :] = jnp.zeros((HALO, EXT_X, LEV), jnp.float32)
    inner = slice(HALO, HALO + TILE_R)
    for d, (size, flag) in enumerate(((ce, ef), (cn, nf))):
        us[d, 0:HALO] = wind_s[d].astype(jnp.float32)
        us[d, HALO + TILE_R :] = wind_n[d].astype(jnp.float32)
        us[d, inner, 0:HALO] = west[d].astype(jnp.float32)
        us[d, inner, HALO + TILE_X :] = east[d].astype(jnp.float32)
        us[d, inner, HALO : HALO + TILE_X] = jnp.where(flag[...] > 0, size[...], -size[...])

    def gains(r, carry):
        for d in range(2):
            speed = jnp.abs(us[d, r])
            gs[d, r] = 0.5 * speed * (1.0 - speed)
        return carry

    lax.fori_loop(0, EXT_R, gains, 0)
    for t in range(1, STEPS + 1):
        old, new = (qa, qb) if t % 2 else (qb, qa)
        low = jnp.where(band == 0, HALO, 2 * t)
        high = jnp.where(band == WAVE - 1, HALO + TILE_R, EXT_R - 2 * t)

        def slope(r):
            here = old[r]
            return minmod(old[r + 1] - here, here - old[r - 1])

        def face(r, low_slope, high_slope):
            return flux(us[1, r], gs[1, r], old[r], old[r + 1], low_slope, high_slope)

        def row(r, carry):
            here_slope, below = carry
            here = old[r]
            next_slope = slope(r + 1)
            above = face(r, here_slope, next_slope)
            right = shifted(here, -1)
            jump = right - here
            steep = minmod(jump, shifted(jump, 1))
            east_face = flux(us[0, r], gs[0, r], here, right, steep, shifted(steep, -1))
            fresh = here - (east_face - shifted(east_face, 1)) - (above - below)
            if t == STEPS:
                out[r - HALO] = fresh[HALO : HALO + TILE_X]
            else:
                new[r] = fresh
            return next_slope, above

        first = slope(low)
        lax.fori_loop(low, high, row, (first, face(low - 1, slope(low - 1), first)))


def advected(band, middle, halo, winds, halos):
    return pl.pallas_call(
        advect_kernel,
        in_specs=[pl.BlockSpec(memory_space=pltpu.SMEM)]
        + [pl.BlockSpec(memory_space=pltpu.VMEM)] * 10,
        out_shape=jax.ShapeDtypeStruct((TILE_R, TILE_X, LEV), jnp.float32),
        scratch_shapes=[
            pltpu.VMEM((EXT_R, EXT_X, LEV), jnp.float32),
            pltpu.VMEM((EXT_R, EXT_X, LEV), jnp.float32),
            pltpu.VMEM((2, EXT_R, EXT_X, LEV), jnp.float32),
            pltpu.VMEM((2, EXT_R, EXT_X, LEV), jnp.float32),
        ],
        compiler_params=PARAMS,
    )(band[None], middle, halo, *winds, *halos)


def from_below(block, axis, wrap):
    pairs = [(i, (i + 1) % 16) for i in range(16 if wrap else 15)]
    return lax.ppermute(block, axis, pairs)


def from_above(block, axis, wrap):
    pairs = [((i + 1) % 16, i) for i in range(16 if wrap else 15)]
    return lax.ppermute(block, axis, pairs)


def per_device(
    control,
    vert_root,
    legendre,
    row_wavenumber,
    courant_east,
    courant_north,
    east_flags,
    north_flags,
):
    lat = lax.axis_index("lat").astype(jnp.int32)
    wave = lax.axis_index("wave").astype(jnp.int32)
    packed = packed_inputs(control, vert_root, legendre, row_wavenumber, lat * ORDERS)
    winds = jnp.stack(
        [
            jnp.where(flag > 0, size, -size).astype(jnp.bfloat16)
            for size, flag in ((courant_east, east_flags), (courant_north, north_flags))
        ]
    )
    west = from_below(winds[:, :, -HALO:], "lat", True)
    east = from_above(winds[:, :, :HALO], "lat", True)
    wide = jnp.concatenate([west, winds, east], axis=2)
    tables = angle_tables()
    packed = lax.all_to_all(packed, "wave", 0, 0, tiled=True)
    packed, wide, tables = lax.optimization_barrier((packed, wide, tables))
    modes = modes_of(packed)
    modes, wide = lax.optimization_barrier((modes, wide))
    wind_s = from_below(wide[:, -HALO:], "wave", False)
    wind_n = from_above(wide[:, :HALO], "wave", False)
    modes = lax.all_to_all(modes.reshape(LATS, SLOTS, LEV), ("wave", "lat"), 0, 0, tiled=True)
    row = latitude_row(modes.reshape(LATS * SLOTS, LEV), tables)
    pairs = []
    for w in range(WAVE):
        for l in range(LAT):
            to = w - 1 if l < HALO else w + 1
            if 0 <= to < WAVE:
                pairs.append((w * LAT + l, to * LAT + l))
    next_row = lax.ppermute(row, ("wave", "lat"), pairs)
    middle = lax.all_to_all(row, "lat", 0, 0, tiled=True)
    halo = lax.all_to_all(next_row, "lat", 0, 0, tiled=True)
    return advected(
        wave,
        middle,
        halo,
        (courant_east, courant_north, east_flags, north_flags),
        (west, east, wind_s, wind_n),
    )


def solution(mesh):
    return jax.shard_map(
        per_device,
        mesh=mesh,
        in_specs=(
            P("wave", "lat", None),
            P("wave", None, None),
            P("lat", "wave", None),
            P("wave"),
            P("wave", "lat", None),
            P("wave", "lat", None),
            P("wave", "lat", None),
            P("wave", "lat", None),
        ),
        out_specs=P("wave", "lat", None),
        check_vma=False,
    )
```

```python
import math

import jax
import jax.numpy as jnp
import numpy as np
from jax import lax
from jax.experimental import pallas as pl
from jax.experimental.pallas import tpu as pltpu
from jax.sharding import PartitionSpec as P

NW = 640
LEV = 128
STEPS = 4
NLON = 2 * NW
WAVE = 16
LAT = 16
ROWS = NW // WAVE
ORDERS = NW // LAT
LATS = 256
TILE_R = LATS // WAVE
TILE_X = NLON // LAT
HALO = 2 * STEPS
EXT_X = TILE_X + 2 * HALO
EXT_R = TILE_R + 2 * HALO
GROUP = 5
SLOTS = 8
ORDER_OF = ((0, 1, 2), (4, 3, 2))
SHARE = 24
SIZE_OF = (ROWS, ROWS, SHARE)
START_OF = (0, ROWS, 2 * ROWS)
PART_ROWS = 2 * ROWS + SHARE
CHUNK = 8
CHUNKS = ROWS // CHUNK
FAR = 16
COLUMNS = 3 * LATS
SOUTH_ROWS = HALO - 1
NORTH_ROWS = HALO - 2
PARAMS = pltpu.CompilerParams(vmem_limit_bytes=24 * 1024 * 1024)


def owned(w, slot):
    order = GROUP * (w // 2) + ORDER_OF[w % 2][slot]
    return order, ROWS - SHARE if slot == 2 and w % 2 else 0, SIZE_OF[slot]


def packing_kernel(
    wavenumber, first, control, vert, legendre, out, cbuf, vbuf, scratch, whole, share, isem, osem
):
    loads = []
    for i in range(CHUNKS):
        rows = pl.ds(i * CHUNK * ORDERS, CHUNK * ORDERS)
        mats = pl.ds(i * CHUNK, CHUNK)
        loads.append(
            (
                pltpu.make_async_copy(control.at[rows], cbuf.at[rows], isem.at[0, i]),
                pltpu.make_async_copy(vert.at[mats], vbuf.at[mats], isem.at[1, i]),
            )
        )
    for pair in loads:
        for load in pair:
            load.start()
    sends = []
    for w in range(WAVE):
        for slot in range(3):
            order, start, size = owned(w, slot)
            sends.append(
                pltpu.make_async_copy(
                    legendre.at[order, pl.ds(start, size)],
                    out.at[w, pl.ds(PART_ROWS + START_OF[slot], size)],
                    osem.at[0, w, slot],
                )
            )
            sends[-1].start()
    row_id = lax.broadcasted_iota(jnp.int32, (2 * LEV, 2 * LEV), 0)
    column = lax.broadcasted_iota(jnp.int32, (2 * LEV, 2 * LEV), 1)
    chosen = column == (row_id & 1) * LEV + (row_id >> 1)
    pick = jnp.where(chosen, 1.0, 0.0).astype(jnp.bfloat16)
    orders = first[0] + lax.broadcasted_iota(jnp.int32, (ORDERS, 2 * LEV), 0)
    for i in range(CHUNKS):
        for load in loads[i]:
            load.wait()
        parts = jnp.dot(
            cbuf[i * CHUNK * ORDERS : (i + 1) * CHUNK * ORDERS],
            pick,
            preferred_element_type=jnp.float32,
        )
        for k in range(CHUNK):
            r = i * CHUNK + k
            rows = jnp.where(wavenumber[r] >= orders, parts[k * ORDERS : (k + 1) * ORDERS], 0.0)
            both = jnp.concatenate([rows[:, :LEV], rows[:, LEV:]], axis=0).astype(jnp.bfloat16)
            mixed = lax.dot_general(
                both, vbuf[r], (((1,), (1,)), ((), ())), preferred_element_type=jnp.float32
            )
            for p in range(2):
                scratch[p, pl.ds(r, ORDERS, stride=ROWS), :] = mixed[p * ORDERS : (p + 1) * ORDERS]
    for w in range(WAVE):
        for slot in range(3):
            order, start, size = owned(w, slot)
            base = order * ROWS + start
            values = jnp.concatenate(
                [scratch[0, base : base + size], scratch[1, base : base + size]], axis=1
            )
            if slot < 2:
                kept = whole.at[w, slot]
            else:
                kept = share.at[w]
                if w % 2:
                    own = lax.broadcasted_iota(jnp.int32, values.shape, 0) >= 2 * SHARE - ROWS
                    values = jnp.where(own, values, 0.0)
            kept[...] = values.astype(jnp.bfloat16)
            sends.append(
                pltpu.make_async_copy(
                    kept, out.at[w, pl.ds(START_OF[slot], size)], osem.at[1, w, slot]
                )
            )
            sends[-1].start()
    for send in sends:
        send.wait()


def packed_inputs(control, vert_root, legendre, row_wavenumber, first_order):
    smem = pl.BlockSpec(memory_space=pltpu.SMEM)
    far = pl.BlockSpec(memory_space=pltpu.HBM)
    return pl.pallas_call(
        packing_kernel,
        in_specs=[smem, smem, far, far, far],
        out_specs=far,
        out_shape=jax.ShapeDtypeStruct((WAVE, 2 * PART_ROWS, 2 * LEV), jnp.bfloat16),
        scratch_shapes=[
            pltpu.VMEM((ROWS * ORDERS, 2 * LEV), jnp.bfloat16),
            pltpu.VMEM((ROWS, LEV, LEV), jnp.bfloat16),
            pltpu.VMEM((2, ORDERS * ROWS, LEV), jnp.float32),
            pltpu.VMEM((WAVE, 2, ROWS, 2 * LEV), jnp.bfloat16),
            pltpu.VMEM((WAVE, SHARE, 2 * LEV), jnp.bfloat16),
            pltpu.SemaphoreType.DMA((2, CHUNKS)),
            pltpu.SemaphoreType.DMA((2, WAVE, 3)),
        ],
    )(
        row_wavenumber,
        first_order[None],
        control.reshape(ROWS * ORDERS, 2 * LEV),
        vert_root,
        legendre,
    )


def modes_kernel(packed, out, left, right, result):
    result[...] = jnp.zeros(result.shape, jnp.float32)
    for slot in range(3):
        size = SIZE_OF[slot]
        for s in range(WAVE):
            rows = slice(s * size, (s + 1) * size)
            for start, side in ((START_OF[slot], right), (PART_ROWS + START_OF[slot], left)):
                block = packed[s, start // 8 : (start + size) // 8].astype(jnp.float32)
                side[rows, :] = block.reshape(size, 2 * LEV)
        total = lax.dot_general(
            left[0 : WAVE * size].astype(jnp.bfloat16),
            right[0 : WAVE * size].astype(jnp.bfloat16),
            (((0,), (0,)), ((), ())),
            preferred_element_type=jnp.float32,
        )
        for p in range(2):
            result[pl.ds(2 * slot + p, LATS, stride=SLOTS), :] = total[:, p * LEV : (p + 1) * LEV]
    out[...] = result[...].astype(jnp.bfloat16)


def modes_of(packed):
    return pl.pallas_call(
        modes_kernel,
        out_shape=jax.ShapeDtypeStruct((LATS * SLOTS, LEV), jnp.bfloat16),
        scratch_shapes=[
            pltpu.VMEM((NW, LATS), jnp.float32),
            pltpu.VMEM((NW, 2 * LEV), jnp.float32),
            pltpu.VMEM((LATS * SLOTS, LEV), jnp.float32),
        ],
        compiler_params=PARAMS,
    )(packed.reshape(WAVE, PART_ROWS // 4, 8, 2 * LEV))


def angle_tables():
    order = np.zeros((3, WAVE, LAT), np.int32)
    for w in range(WAVE):
        for slot in range(3):
            order[slot, w] = np.arange(LAT) * ORDERS + owned(w, slot)[0]
    order = jnp.asarray(order.reshape(-1))
    weight = jnp.where(order == 0, 1.0, 2.0).astype(jnp.float32) * (1.0 / math.sqrt(NLON))

    def turn(steps):
        return (steps % NLON).astype(jnp.float32) * (2.0 * math.pi / NLON)

    local = jnp.arange(EXT_X, dtype=jnp.int32) - HALO + NLON
    near = turn(order[None, :] * local[:, None])
    far = turn(order[None, :] * (TILE_X * jnp.arange(FAR, dtype=jnp.int32))[:, None])
    return jnp.concatenate(
        [weight * jnp.cos(near), -weight * jnp.sin(near), jnp.cos(far), jnp.sin(far)]
    )


def fourier_kernel(modes, local, out, wide, rhs):
    wide[...] = modes[...].astype(jnp.float32)
    for p in range(2):
        for slot in range(3):
            rows = wide[pl.ds(2 * slot + p, LATS, stride=SLOTS), :]
            start = p * COLUMNS + slot * LATS
            rhs[start : start + LATS] = rows.astype(jnp.bfloat16)

    def put(band, real, imaginary):
        basis = jnp.concatenate(
            [real.astype(jnp.bfloat16), imaginary.astype(jnp.bfloat16)], axis=1
        )
        total = jnp.dot(basis, rhs[...], preferred_element_type=jnp.float32)
        out[band] = total.astype(jnp.bfloat16)

    for b in range(LAT // 2 + 1):
        far_cos = local[2 * EXT_X + b : 2 * EXT_X + b + 1, :]
        far_sin = local[2 * EXT_X + FAR + b : 2 * EXT_X + FAR + b + 1, :]
        near_cos, near_sin = local[0:EXT_X], local[EXT_X : 2 * EXT_X]
        cc, ss = far_cos * near_cos, far_sin * near_sin
        cs, sc = far_cos * near_sin, far_sin * near_cos
        put(b, cc + ss, cs - sc)
        if 0 < b < LAT // 2:
            put(LAT - b, cc - ss, cs + sc)


def latitude_row(modes, tables):
    return pl.pallas_call(
        fourier_kernel,
        out_shape=jax.ShapeDtypeStruct((LAT, EXT_X, LEV), jnp.bfloat16),
        scratch_shapes=[
            pltpu.VMEM((LATS * SLOTS, LEV), jnp.float32),
            pltpu.VMEM((2 * COLUMNS, LEV), jnp.bfloat16),
        ],
    )(modes, tables)


def minmod(a, b):
    return jnp.maximum(jnp.minimum(a, b), jnp.minimum(jnp.maximum(a, b), 0.0))


def shifted(array, amount):
    return pltpu.roll(array, amount % array.shape[0], 0)


def flux(wind, gain, low, high, low_slope, high_slope):
    forward = wind > 0.0
    return wind * jnp.where(forward, low, high) + gain * jnp.where(forward, low_slope, high_slope)


def advect_kernel(
    where, middle, halo, ce, cn, ef, nf, west, east, wind_s, wind_n, out, qa, qb, us, gs
):
    band = where[0]
    qa[0:HALO] = halo[HALO:].astype(jnp.float32)
    qa[HALO : HALO + TILE_R] = middle[...].astype(jnp.float32)
    qa[HALO + TILE_R :] = halo[:HALO].astype(jnp.float32)
    qb[0:HALO] = jnp.zeros((HALO, EXT_X, LEV), jnp.float32)
    qb[HALO + TILE_R :] = jnp.zeros((HALO, EXT_X, LEV), jnp.float32)
    inner = slice(HALO, HALO + TILE_R)
    for d, (size, flag) in enumerate(((ce, ef), (cn, nf))):
        us[d, HALO - SOUTH_ROWS : HALO] = wind_s[d].astype(jnp.float32)
        us[d, HALO + TILE_R : HALO + TILE_R + NORTH_ROWS] = wind_n[d].astype(jnp.float32)
        us[d, inner, 0:HALO] = west[d].astype(jnp.float32)
        us[d, inner, HALO + TILE_X :] = east[d].astype(jnp.float32)
        us[d, inner, HALO : HALO + TILE_X] = jnp.where(flag[...] > 0, size[...], -size[...])

    def gains(r, carry):
        for d in range(2):
            speed = jnp.abs(us[d, r])
            gs[d, r] = 0.5 * speed * (1.0 - speed)
        return carry

    lax.fori_loop(HALO - SOUTH_ROWS, HALO + TILE_R + NORTH_ROWS, gains, 0)
    for t in range(1, STEPS + 1):
        old, new = (qa, qb) if t % 2 else (qb, qa)
        low = jnp.where(band == 0, HALO, 2 * t)
        high = jnp.where(band == WAVE - 1, HALO + TILE_R, EXT_R - 2 * t)

        def slope(r):
            here = old[r]
            return minmod(old[r + 1] - here, here - old[r - 1])

        def face(r, low_slope, high_slope):
            return flux(us[1, r], gs[1, r], old[r], old[r + 1], low_slope, high_slope)

        def row(r, carry):
            here_slope, below = carry
            here = old[r]
            next_slope = slope(r + 1)
            above = face(r, here_slope, next_slope)
            right = shifted(here, -1)
            jump = right - here
            steep = minmod(jump, shifted(jump, 1))
            east_face = flux(us[0, r], gs[0, r], here, right, steep, shifted(steep, -1))
            fresh = here - (east_face - shifted(east_face, 1)) - (above - below)
            if t == STEPS:
                out[r - HALO] = fresh[HALO : HALO + TILE_X]
            else:
                new[r] = fresh
            return next_slope, above

        first = slope(low)
        lax.fori_loop(low, high, row, (first, face(low - 1, slope(low - 1), first)))


def advected(band, middle, halo, winds, halos):
    return pl.pallas_call(
        advect_kernel,
        in_specs=[pl.BlockSpec(memory_space=pltpu.SMEM)]
        + [pl.BlockSpec(memory_space=pltpu.VMEM)] * 10,
        out_shape=jax.ShapeDtypeStruct((TILE_R, TILE_X, LEV), jnp.float32),
        scratch_shapes=[
            pltpu.VMEM((EXT_R, EXT_X, LEV), jnp.float32),
            pltpu.VMEM((EXT_R, EXT_X, LEV), jnp.float32),
            pltpu.VMEM((2, EXT_R, EXT_X, LEV), jnp.float32),
            pltpu.VMEM((2, EXT_R, EXT_X, LEV), jnp.float32),
        ],
        compiler_params=PARAMS,
    )(band[None], middle, halo, *winds, *halos)


def from_below(block, axis, wrap):
    pairs = [(i, (i + 1) % 16) for i in range(16 if wrap else 15)]
    return lax.ppermute(block, axis, pairs)


def from_above(block, axis, wrap):
    pairs = [((i + 1) % 16, i) for i in range(16 if wrap else 15)]
    return lax.ppermute(block, axis, pairs)


def per_device(
    control,
    vert_root,
    legendre,
    row_wavenumber,
    courant_east,
    courant_north,
    east_flags,
    north_flags,
):
    lat = lax.axis_index("lat").astype(jnp.int32)
    wave = lax.axis_index("wave").astype(jnp.int32)
    packed = packed_inputs(control, vert_root, legendre, row_wavenumber, lat * ORDERS)
    winds = jnp.stack(
        [
            jnp.where(flag > 0, size, -size).astype(jnp.bfloat16)
            for size, flag in ((courant_east, east_flags), (courant_north, north_flags))
        ]
    )
    west = from_below(winds[:, :, -HALO:], "lat", True)
    east = from_above(winds[:, :, :HALO], "lat", True)
    wide = jnp.concatenate([west, winds, east], axis=2)
    tables = angle_tables()
    packed = lax.all_to_all(packed, "wave", 0, 0, tiled=True)
    packed, wide, tables = lax.optimization_barrier((packed, wide, tables))
    modes = modes_of(packed)
    modes, wide = lax.optimization_barrier((modes, wide))
    wind_s = from_below(wide[:, -SOUTH_ROWS:], "wave", False)
    wind_n = from_above(wide[:, :NORTH_ROWS], "wave", False)
    modes = lax.all_to_all(modes.reshape(LATS, SLOTS, LEV), ("wave", "lat"), 0, 0, tiled=True)
    row = latitude_row(modes.reshape(LATS * SLOTS, LEV), tables)
    pairs = []
    for w in range(WAVE):
        for l in range(LAT):
            to = w - 1 if l < HALO else w + 1
            if 0 <= to < WAVE:
                pairs.append((w * LAT + l, to * LAT + l))
    next_row = lax.ppermute(row, ("wave", "lat"), pairs)
    middle = lax.all_to_all(row, "lat", 0, 0, tiled=True)
    halo = lax.all_to_all(next_row, "lat", 0, 0, tiled=True)
    return advected(
        wave,
        middle,
        halo,
        (courant_east, courant_north, east_flags, north_flags),
        (west, east, wind_s, wind_n),
    )


def solution(mesh):
    return jax.shard_map(
        per_device,
        mesh=mesh,
        in_specs=(
            P("wave", "lat", None),
            P("wave", None, None),
            P("lat", "wave", None),
            P("wave"),
            P("wave", "lat", None),
            P("wave", "lat", None),
            P("wave", "lat", None),
            P("wave", "lat", None),
        ),
        out_specs=P("wave", "lat", None),
        check_vma=False,
    )
```

```python
import math

import jax
import jax.numpy as jnp
import numpy as np
from jax import lax
from jax.experimental import pallas as pl
from jax.experimental.pallas import tpu as pltpu
from jax.sharding import PartitionSpec as P

NW = 640
LEV = 128
STEPS = 4
NLON = 2 * NW
WAVE = 16
LAT = 16
ROWS = NW // WAVE
ORDERS = NW // LAT
LATS = 256
TILE_R = LATS // WAVE
TILE_X = NLON // LAT
HALO = 2 * STEPS
EXT_X = TILE_X + 2 * HALO
EXT_R = TILE_R + 2 * HALO
GROUP = 5
SLOTS = 8
ORDER_OF = ((0, 1, 2), (4, 3, 2))
SHARE = 24
SIZE_OF = (ROWS, ROWS, SHARE)
START_OF = (0, ROWS, 2 * ROWS)
PART_ROWS = 2 * ROWS + SHARE
CHUNK = 8
CHUNKS = ROWS // CHUNK
FAR = 16
COLUMNS = 3 * LATS
SOUTH_ROWS = HALO - 1
NORTH_ROWS = HALO - 2
PARAMS = pltpu.CompilerParams(vmem_limit_bytes=24 * 1024 * 1024)


def owned(w, slot):
    order = GROUP * (w // 2) + ORDER_OF[w % 2][slot]
    return order, ROWS - SHARE if slot == 2 and w % 2 else 0, SIZE_OF[slot]


def packing_kernel(
    wavenumber, first, control, vert, legendre, out, cbuf, vbuf, lbuf, scratch, whole, share, isem, osem
):
    loads = []
    for i in range(CHUNKS):
        rows = pl.ds(i * CHUNK * ORDERS, CHUNK * ORDERS)
        mats = pl.ds(i * CHUNK, CHUNK)
        loads.append(
            (
                pltpu.make_async_copy(legendre.at[mats], lbuf.at[mats], isem.at[2, i]),
                pltpu.make_async_copy(control.at[rows], cbuf.at[rows], isem.at[0, i]),
                pltpu.make_async_copy(vert.at[mats], vbuf.at[mats], isem.at[1, i]),
            )
        )
    for several in loads:
        for load in several[1:]:
            load.start()
    for several in loads:
        several[0].start()
    sends = []
    row_id = lax.broadcasted_iota(jnp.int32, (2 * LEV, 2 * LEV), 0)
    column = lax.broadcasted_iota(jnp.int32, (2 * LEV, 2 * LEV), 1)
    chosen = column == (row_id & 1) * LEV + (row_id >> 1)
    pick = jnp.where(chosen, 1.0, 0.0).astype(jnp.bfloat16)
    orders = first[0] + lax.broadcasted_iota(jnp.int32, (ORDERS, 2 * LEV), 0)
    for i in range(CHUNKS):
        for load in loads[i][1:]:
            load.wait()
        parts = jnp.dot(
            cbuf[i * CHUNK * ORDERS : (i + 1) * CHUNK * ORDERS],
            pick,
            preferred_element_type=jnp.float32,
        )
        for k in range(CHUNK):
            r = i * CHUNK + k
            rows = jnp.where(wavenumber[r] >= orders, parts[k * ORDERS : (k + 1) * ORDERS], 0.0)
            both = jnp.concatenate([rows[:, :LEV], rows[:, LEV:]], axis=0).astype(jnp.bfloat16)
            mixed = lax.dot_general(
                both, vbuf[r], (((1,), (1,)), ((), ())), preferred_element_type=jnp.float32
            )
            for p in range(2):
                scratch[p, pl.ds(r, ORDERS, stride=ROWS), :] = mixed[p * ORDERS : (p + 1) * ORDERS]
    for several in loads:
        several[0].wait()
    for w in range(WAVE):
        for slot in range(3):
            order, start, size = owned(w, slot)
            sends.append(
                pltpu.make_async_copy(
                    lbuf.at[order, pl.ds(start, size)],
                    out.at[w, pl.ds(PART_ROWS + START_OF[slot], size)],
                    osem.at[0, w, slot],
                )
            )
            sends[-1].start()
    for w in range(WAVE):
        for slot in range(3):
            order, start, size = owned(w, slot)
            base = order * ROWS + start
            values = jnp.concatenate(
                [scratch[0, base : base + size], scratch[1, base : base + size]], axis=1
            )
            if slot < 2:
                kept = whole.at[w, slot]
            else:
                kept = share.at[w]
                if w % 2:
                    own = lax.broadcasted_iota(jnp.int32, values.shape, 0) >= 2 * SHARE - ROWS
                    values = jnp.where(own, values, 0.0)
            kept[...] = values.astype(jnp.bfloat16)
            sends.append(
                pltpu.make_async_copy(
                    kept, out.at[w, pl.ds(START_OF[slot], size)], osem.at[1, w, slot]
                )
            )
            sends[-1].start()
    for send in sends:
        send.wait()


def packed_inputs(control, vert_root, legendre, row_wavenumber, first_order):
    smem = pl.BlockSpec(memory_space=pltpu.SMEM)
    far = pl.BlockSpec(memory_space=pltpu.HBM)
    return pl.pallas_call(
        packing_kernel,
        in_specs=[smem, smem, far, far, far],
        out_specs=far,
        out_shape=jax.ShapeDtypeStruct((WAVE, 2 * PART_ROWS, 2 * LEV), jnp.bfloat16),
        scratch_shapes=[
            pltpu.VMEM((ROWS * ORDERS, 2 * LEV), jnp.bfloat16),
            pltpu.VMEM((ROWS, LEV, LEV), jnp.bfloat16),
            pltpu.VMEM((ORDERS, ROWS, LATS), jnp.bfloat16),
            pltpu.VMEM((2, ORDERS * ROWS, LEV), jnp.float32),
            pltpu.VMEM((WAVE, 2, ROWS, 2 * LEV), jnp.bfloat16),
            pltpu.VMEM((WAVE, SHARE, 2 * LEV), jnp.bfloat16),
            pltpu.SemaphoreType.DMA((3, CHUNKS)),
            pltpu.SemaphoreType.DMA((2, WAVE, 3)),
        ],
    )(
        row_wavenumber,
        first_order[None],
        control.reshape(ROWS * ORDERS, 2 * LEV),
        vert_root,
        legendre,
    )


def modes_kernel(packed, out, left, right, result):
    result[...] = jnp.zeros(result.shape, jnp.float32)
    for slot in range(3):
        size = SIZE_OF[slot]
        for s in range(WAVE):
            rows = slice(s * size, (s + 1) * size)
            for start, side in ((START_OF[slot], right), (PART_ROWS + START_OF[slot], left)):
                block = packed[s, start // 8 : (start + size) // 8].astype(jnp.float32)
                side[rows, :] = block.reshape(size, 2 * LEV)
        total = lax.dot_general(
            left[0 : WAVE * size].astype(jnp.bfloat16),
            right[0 : WAVE * size].astype(jnp.bfloat16),
            (((0,), (0,)), ((), ())),
            preferred_element_type=jnp.float32,
        )
        for p in range(2):
            result[pl.ds(2 * slot + p, LATS, stride=SLOTS), :] = total[:, p * LEV : (p + 1) * LEV]
    out[...] = result[...].astype(jnp.bfloat16)


def modes_of(packed):
    return pl.pallas_call(
        modes_kernel,
        out_shape=jax.ShapeDtypeStruct((LATS * SLOTS, LEV), jnp.bfloat16),
        scratch_shapes=[
            pltpu.VMEM((NW, LATS), jnp.float32),
            pltpu.VMEM((NW, 2 * LEV), jnp.float32),
            pltpu.VMEM((LATS * SLOTS, LEV), jnp.float32),
        ],
        compiler_params=PARAMS,
    )(packed.reshape(WAVE, PART_ROWS // 4, 8, 2 * LEV))


def angle_tables():
    order = np.zeros((3, WAVE, LAT), np.int32)
    for w in range(WAVE):
        for slot in range(3):
            order[slot, w] = np.arange(LAT) * ORDERS + owned(w, slot)[0]
    order = jnp.asarray(order.reshape(-1))
    weight = jnp.where(order == 0, 1.0, 2.0).astype(jnp.float32) * (1.0 / math.sqrt(NLON))

    def turn(steps):
        return (steps % NLON).astype(jnp.float32) * (2.0 * math.pi / NLON)

    local = jnp.arange(EXT_X, dtype=jnp.int32) - HALO + NLON
    near = turn(order[None, :] * local[:, None])
    far = turn(order[None, :] * (TILE_X * jnp.arange(FAR, dtype=jnp.int32))[:, None])
    return jnp.concatenate(
        [weight * jnp.cos(near), -weight * jnp.sin(near), jnp.cos(far), jnp.sin(far)]
    )


def fourier_kernel(modes, tables, out, held, local, wide, rhs, bands, isem, osem):
    load_modes = pltpu.make_async_copy(modes, held, isem.at[0])
    load_tables = pltpu.make_async_copy(tables, local, isem.at[1])
    load_modes.start()
    load_tables.start()
    load_modes.wait()
    wide[...] = held[...].astype(jnp.float32)
    for p in range(2):
        for slot in range(3):
            rows = wide[pl.ds(2 * slot + p, LATS, stride=SLOTS), :]
            start = p * COLUMNS + slot * LATS
            rhs[start : start + LATS] = rows.astype(jnp.bfloat16)
    load_tables.wait()
    sends = []

    def put(band, real, imaginary):
        basis = jnp.concatenate(
            [real.astype(jnp.bfloat16), imaginary.astype(jnp.bfloat16)], axis=1
        )
        total = jnp.dot(basis, rhs[...], preferred_element_type=jnp.float32)
        bands[band] = total.astype(jnp.bfloat16)
        sends.append(pltpu.make_async_copy(bands.at[band], out.at[band], osem.at[band]))
        sends[-1].start()

    for b in range(LAT // 2 + 1):
        far_cos = local[2 * EXT_X + b : 2 * EXT_X + b + 1, :]
        far_sin = local[2 * EXT_X + FAR + b : 2 * EXT_X + FAR + b + 1, :]
        near_cos, near_sin = local[0:EXT_X], local[EXT_X : 2 * EXT_X]
        cc, ss = far_cos * near_cos, far_sin * near_sin
        cs, sc = far_cos * near_sin, far_sin * near_cos
        put(b, cc + ss, cs - sc)
        if 0 < b < LAT // 2:
            put(LAT - b, cc - ss, cs + sc)
    for send in sends:
        send.wait()


def latitude_row(modes, tables):
    far = pl.BlockSpec(memory_space=pltpu.HBM)
    return pl.pallas_call(
        fourier_kernel,
        in_specs=[far, far],
        out_specs=far,
        out_shape=jax.ShapeDtypeStruct((LAT, EXT_X, LEV), jnp.bfloat16),
        scratch_shapes=[
            pltpu.VMEM((LATS * SLOTS, LEV), jnp.bfloat16),
            pltpu.VMEM((2 * EXT_X + 2 * FAR, COLUMNS), jnp.float32),
            pltpu.VMEM((LATS * SLOTS, LEV), jnp.float32),
            pltpu.VMEM((2 * COLUMNS, LEV), jnp.bfloat16),
            pltpu.VMEM((LAT, EXT_X, LEV), jnp.bfloat16),
            pltpu.SemaphoreType.DMA((2,)),
            pltpu.SemaphoreType.DMA((LAT,)),
        ],
    )(modes, tables)


def minmod(a, b):
    return jnp.maximum(jnp.minimum(a, b), jnp.minimum(jnp.maximum(a, b), 0.0))


def shifted(array, amount):
    return pltpu.roll(array, amount % array.shape[0], 0)


def flux(wind, gain, low, high, low_slope, high_slope):
    forward = wind > 0.0
    return wind * jnp.where(forward, low, high) + gain * jnp.where(forward, low_slope, high_slope)


def advect_kernel(
    where, middle, halo, ce, cn, ef, nf, west, east, wind_s, wind_n, out, qa, qb, us, gs
):
    band = where[0]
    qa[0:HALO] = halo[HALO:].astype(jnp.float32)
    qa[HALO : HALO + TILE_R] = middle[...].astype(jnp.float32)
    qa[HALO + TILE_R :] = halo[:HALO].astype(jnp.float32)
    qb[0:HALO] = jnp.zeros((HALO, EXT_X, LEV), jnp.float32)
    qb[HALO + TILE_R :] = jnp.zeros((HALO, EXT_X, LEV), jnp.float32)
    inner = slice(HALO, HALO + TILE_R)
    for d, (size, flag) in enumerate(((ce, ef), (cn, nf))):
        us[d, HALO - SOUTH_ROWS : HALO] = wind_s[d].astype(jnp.float32)
        us[d, HALO + TILE_R : HALO + TILE_R + NORTH_ROWS] = wind_n[d].astype(jnp.float32)
        us[d, inner, 0:HALO] = west[d].astype(jnp.float32)
        us[d, inner, HALO + TILE_X :] = east[d].astype(jnp.float32)
        us[d, inner, HALO : HALO + TILE_X] = jnp.where(flag[...] > 0, size[...], -size[...])

    def gains(r, carry):
        for d in range(2):
            speed = jnp.abs(us[d, r])
            gs[d, r] = 0.5 * speed * (1.0 - speed)
        return carry

    lax.fori_loop(HALO - SOUTH_ROWS, HALO + TILE_R + NORTH_ROWS, gains, 0)
    for t in range(1, STEPS + 1):
        old, new = (qa, qb) if t % 2 else (qb, qa)
        low = jnp.where(band == 0, HALO, 2 * t)
        high = jnp.where(band == WAVE - 1, HALO + TILE_R, EXT_R - 2 * t)

        def slope(r):
            here = old[r]
            return minmod(old[r + 1] - here, here - old[r - 1])

        def face(r, low_slope, high_slope):
            return flux(us[1, r], gs[1, r], old[r], old[r + 1], low_slope, high_slope)

        def row(r, carry):
            here_slope, below = carry
            here = old[r]
            next_slope = slope(r + 1)
            above = face(r, here_slope, next_slope)
            right = shifted(here, -1)
            jump = right - here
            steep = minmod(jump, shifted(jump, 1))
            east_face = flux(us[0, r], gs[0, r], here, right, steep, shifted(steep, -1))
            fresh = here - (east_face - shifted(east_face, 1)) - (above - below)
            if t == STEPS:
                out[r - HALO] = fresh[HALO : HALO + TILE_X]
            else:
                new[r] = fresh
            return next_slope, above

        first = slope(low)
        lax.fori_loop(low, high, row, (first, face(low - 1, slope(low - 1), first)))


def advected(band, middle, halo, winds, halos):
    return pl.pallas_call(
        advect_kernel,
        in_specs=[pl.BlockSpec(memory_space=pltpu.SMEM)]
        + [pl.BlockSpec(memory_space=pltpu.VMEM)] * 10,
        out_shape=jax.ShapeDtypeStruct((TILE_R, TILE_X, LEV), jnp.float32),
        scratch_shapes=[
            pltpu.VMEM((EXT_R, EXT_X, LEV), jnp.float32),
            pltpu.VMEM((EXT_R, EXT_X, LEV), jnp.float32),
            pltpu.VMEM((2, EXT_R, EXT_X, LEV), jnp.float32),
            pltpu.VMEM((2, EXT_R, EXT_X, LEV), jnp.float32),
        ],
        compiler_params=PARAMS,
    )(band[None], middle, halo, *winds, *halos)


def from_below(block, axis, wrap):
    pairs = [(i, (i + 1) % 16) for i in range(16 if wrap else 15)]
    return lax.ppermute(block, axis, pairs)


def from_above(block, axis, wrap):
    pairs = [((i + 1) % 16, i) for i in range(16 if wrap else 15)]
    return lax.ppermute(block, axis, pairs)


def per_device(
    control,
    vert_root,
    legendre,
    row_wavenumber,
    courant_east,
    courant_north,
    east_flags,
    north_flags,
):
    lat = lax.axis_index("lat").astype(jnp.int32)
    wave = lax.axis_index("wave").astype(jnp.int32)
    packed = packed_inputs(control, vert_root, legendre, row_wavenumber, lat * ORDERS)
    winds = jnp.stack(
        [
            jnp.where(flag > 0, size, -size).astype(jnp.bfloat16)
            for size, flag in ((courant_east, east_flags), (courant_north, north_flags))
        ]
    )
    west = from_below(winds[:, :, -HALO:], "lat", True)
    east = from_above(winds[:, :, :HALO], "lat", True)
    wide = jnp.concatenate([west, winds, east], axis=2)
    tables = angle_tables()
    packed = lax.all_to_all(packed, "wave", 0, 0, tiled=True)
    upper, lower = wide[:, -SOUTH_ROWS:], wide[:, :NORTH_ROWS]
    packed, upper, lower, tables = lax.optimization_barrier((packed, upper, lower, tables))
    modes = modes_of(packed)
    modes, upper, lower = lax.optimization_barrier((modes, upper, lower))
    wind_s = from_below(upper, "wave", False)
    wind_n = from_above(lower, "wave", False)
    modes = lax.all_to_all(modes.reshape(LATS, SLOTS, LEV), ("wave", "lat"), 0, 0, tiled=True)
    row = latitude_row(modes.reshape(LATS * SLOTS, LEV), tables)
    pairs = []
    for w in range(WAVE):
        for l in range(LAT):
            to = w - 1 if l < HALO else w + 1
            if 0 <= to < WAVE:
                pairs.append((w * LAT + l, to * LAT + l))
    next_row = lax.ppermute(row, ("wave", "lat"), pairs)
    middle = lax.all_to_all(row, "lat", 0, 0, tiled=True)
    halo = lax.all_to_all(next_row, "lat", 0, 0, tiled=True)
    return advected(
        wave,
        middle,
        halo,
        (courant_east, courant_north, east_flags, north_flags),
        (west, east, wind_s, wind_n),
    )


def solution(mesh):
    return jax.shard_map(
        per_device,
        mesh=mesh,
        in_specs=(
            P("wave", "lat", None),
            P("wave", None, None),
            P("lat", "wave", None),
            P("wave"),
            P("wave", "lat", None),
            P("wave", "lat", None),
            P("wave", "lat", None),
            P("wave", "lat", None),
        ),
        out_specs=P("wave", "lat", None),
        check_vma=False,
    )
```

```python
import math

import jax
import jax.numpy as jnp
import numpy as np
from jax import lax
from jax.experimental import pallas as pl
from jax.experimental.pallas import tpu as pltpu
from jax.sharding import PartitionSpec as P

NW = 640
LEV = 128
STEPS = 4
NLON = 2 * NW
WAVE = 16
LAT = 16
ROWS = NW // WAVE
ORDERS = NW // LAT
LATS = 256
TILE_R = LATS // WAVE
TILE_X = NLON // LAT
HALO = 2 * STEPS
EXT_X = TILE_X + 2 * HALO
EXT_R = TILE_R + 2 * HALO
GROUP = 5
SLOTS = 8
ORDER_OF = ((0, 1, 2), (4, 3, 2))
SHARE = 24
SIZE_OF = (ROWS, ROWS, SHARE)
START_OF = (0, ROWS, 2 * ROWS)
PART_ROWS = 2 * ROWS + SHARE
CHUNK = 8
CHUNKS = ROWS // CHUNK
FAR = 8
COLUMNS = 3 * LATS
SOUTH_ROWS = HALO - 1
NORTH_ROWS = HALO - 2
PARAMS = pltpu.CompilerParams(vmem_limit_bytes=24 * 1024 * 1024)


def owned(w, slot):
    order = GROUP * (w // 2) + ORDER_OF[w % 2][slot]
    return order, ROWS - SHARE if slot == 2 and w % 2 else 0, SIZE_OF[slot]


def packing_kernel(
    wavenumber, first, control, vert, legendre, out, cbuf, vbuf, lbuf, scratch, whole, share, isem, osem
):
    loads = []
    for i in range(CHUNKS):
        rows = pl.ds(i * CHUNK * ORDERS, CHUNK * ORDERS)
        mats = pl.ds(i * CHUNK, CHUNK)
        loads.append(
            (
                pltpu.make_async_copy(legendre.at[mats], lbuf.at[mats], isem.at[2, i]),
                pltpu.make_async_copy(control.at[rows], cbuf.at[rows], isem.at[0, i]),
                pltpu.make_async_copy(vert.at[mats], vbuf.at[mats], isem.at[1, i]),
            )
        )
    for several in loads:
        for load in several[1:]:
            load.start()
    for several in loads:
        several[0].start()
    sends = []
    row_id = lax.broadcasted_iota(jnp.int32, (2 * LEV, 2 * LEV), 0)
    column = lax.broadcasted_iota(jnp.int32, (2 * LEV, 2 * LEV), 1)
    chosen = column == (row_id & 1) * LEV + (row_id >> 1)
    pick = jnp.where(chosen, 1.0, 0.0).astype(jnp.bfloat16)
    orders = first[0] + lax.broadcasted_iota(jnp.int32, (ORDERS, 2 * LEV), 0)
    for i in range(CHUNKS):
        for load in loads[i][1:]:
            load.wait()
        parts = jnp.dot(
            cbuf[i * CHUNK * ORDERS : (i + 1) * CHUNK * ORDERS],
            pick,
            preferred_element_type=jnp.float32,
        )
        for k in range(CHUNK):
            r = i * CHUNK + k
            rows = jnp.where(wavenumber[r] >= orders, parts[k * ORDERS : (k + 1) * ORDERS], 0.0)
            both = jnp.concatenate([rows[:, :LEV], rows[:, LEV:]], axis=0).astype(jnp.bfloat16)
            mixed = lax.dot_general(
                both, vbuf[r], (((1,), (1,)), ((), ())), preferred_element_type=jnp.float32
            )
            for p in range(2):
                scratch[p, pl.ds(r, ORDERS, stride=ROWS), :] = mixed[p * ORDERS : (p + 1) * ORDERS]
        loads[i][0].wait()
        for w in range(WAVE):
            for slot in range(3):
                order, start, size = owned(w, slot)
                if order // CHUNK == i:
                    send = pltpu.make_async_copy(
                        lbuf.at[order, pl.ds(start, size)],
                        out.at[w, pl.ds(PART_ROWS + START_OF[slot], size)],
                        osem.at[0, w, slot],
                    )
                    send.start()
                    sends.append(send)
    for w in range(WAVE):
        for slot in range(3):
            order, start, size = owned(w, slot)
            base = order * ROWS + start
            values = jnp.concatenate(
                [scratch[0, base : base + size], scratch[1, base : base + size]], axis=1
            )
            if slot < 2:
                kept = whole.at[w, slot]
            else:
                kept = share.at[w]
                if w % 2:
                    own = lax.broadcasted_iota(jnp.int32, values.shape, 0) >= 2 * SHARE - ROWS
                    values = jnp.where(own, values, 0.0)
            kept[...] = values.astype(jnp.bfloat16)
            sends.append(
                pltpu.make_async_copy(
                    kept, out.at[w, pl.ds(START_OF[slot], size)], osem.at[1, w, slot]
                )
            )
            sends[-1].start()
    for send in sends:
        send.wait()


def packed_inputs(control, vert_root, legendre, row_wavenumber, first_order):
    smem = pl.BlockSpec(memory_space=pltpu.SMEM)
    far = pl.BlockSpec(memory_space=pltpu.HBM)
    return pl.pallas_call(
        packing_kernel,
        in_specs=[smem, smem, far, far, far],
        out_specs=far,
        out_shape=jax.ShapeDtypeStruct((WAVE, 2 * PART_ROWS, 2 * LEV), jnp.bfloat16),
        scratch_shapes=[
            pltpu.VMEM((ROWS * ORDERS, 2 * LEV), jnp.bfloat16),
            pltpu.VMEM((ROWS, LEV, LEV), jnp.bfloat16),
            pltpu.VMEM((ORDERS, ROWS, LATS), jnp.bfloat16),
            pltpu.VMEM((2, ORDERS * ROWS, LEV), jnp.float32),
            pltpu.VMEM((WAVE, 2, ROWS, 2 * LEV), jnp.bfloat16),
            pltpu.VMEM((WAVE, SHARE, 2 * LEV), jnp.bfloat16),
            pltpu.SemaphoreType.DMA((3, CHUNKS)),
            pltpu.SemaphoreType.DMA((2, WAVE, 3)),
        ],
    )(
        row_wavenumber,
        first_order[None],
        control.reshape(ROWS * ORDERS, 2 * LEV),
        vert_root,
        legendre,
    )


def modes_kernel(packed, out, left, right, result):
    result[...] = jnp.zeros(result.shape, jnp.float32)
    for slot in range(3):
        size = SIZE_OF[slot]
        for s in range(WAVE):
            rows = slice(s * size, (s + 1) * size)
            for start, side in ((START_OF[slot], right), (PART_ROWS + START_OF[slot], left)):
                block = packed[s, start // 8 : (start + size) // 8].astype(jnp.float32)
                side[rows, :] = block.reshape(size, 2 * LEV)
        total = lax.dot_general(
            left[0 : WAVE * size].astype(jnp.bfloat16),
            right[0 : WAVE * size].astype(jnp.bfloat16),
            (((0,), (0,)), ((), ())),
            preferred_element_type=jnp.float32,
        )
        for p in range(2):
            result[pl.ds(2 * slot + p, LATS, stride=SLOTS), :] = total[:, p * LEV : (p + 1) * LEV]
    out[...] = result[...].astype(jnp.bfloat16)


def modes_of(packed):
    return pl.pallas_call(
        modes_kernel,
        out_shape=jax.ShapeDtypeStruct((LATS * SLOTS, LEV), jnp.bfloat16),
        scratch_shapes=[
            pltpu.VMEM((NW, LATS), jnp.float32),
            pltpu.VMEM((NW, 2 * LEV), jnp.float32),
            pltpu.VMEM((LATS * SLOTS, LEV), jnp.float32),
        ],
        compiler_params=PARAMS,
    )(packed.reshape(WAVE, PART_ROWS // 4, 8, 2 * LEV))


def angle_tables():
    order = np.zeros((3, WAVE, LAT), np.int32)
    for w in range(WAVE):
        for slot in range(3):
            order[slot, w] = np.arange(LAT) * ORDERS + owned(w, slot)[0]
    order = jnp.asarray(order.reshape(-1))
    weight = jnp.where(order == 0, 1.0, 2.0).astype(jnp.float32) * (1.0 / math.sqrt(NLON))

    def turn(steps):
        return (steps % NLON).astype(jnp.float32) * (2.0 * math.pi / NLON)

    local = jnp.arange(EXT_X, dtype=jnp.int32) - HALO + NLON
    near = turn(order[None, :] * local[:, None])
    far = turn(order[None, :] * (TILE_X * jnp.arange(FAR, dtype=jnp.int32))[:, None])
    return jnp.concatenate(
        [weight * jnp.cos(near), -weight * jnp.sin(near), jnp.cos(far), jnp.sin(far)]
    )


def fourier_kernel(modes, tables, out, held, local, wide, rhs, bands, isem, osem):
    load_modes = pltpu.make_async_copy(modes, held, isem.at[0])
    load_tables = pltpu.make_async_copy(tables, local, isem.at[1])
    load_modes.start()
    load_tables.start()
    load_modes.wait()
    wide[...] = held[...].astype(jnp.float32)
    group = lax.broadcasted_iota(jnp.int32, (LATS, LEV), 0) // (2 * LAT)
    for slot in range(3):
        even = (group + ORDER_OF[0][slot]) % 2 == 0
        for p in range(2):
            rows = wide[pl.ds(2 * slot + p, LATS, stride=SLOTS), :]
            start = p * COLUMNS + slot * LATS
            rhs[start : start + LATS, :LEV] = rows.astype(jnp.bfloat16)
            rhs[start : start + LATS, LEV:] = jnp.where(even, rows, -rows).astype(jnp.bfloat16)
    load_tables.wait()
    sends = []

    def put(band, real, imaginary):
        basis = jnp.concatenate(
            [real.astype(jnp.bfloat16), imaginary.astype(jnp.bfloat16)], axis=1
        )
        total = jnp.dot(basis, rhs[...], preferred_element_type=jnp.float32).astype(jnp.bfloat16)
        for half in range(2):
            place = (band + half * (LAT // 2)) % LAT
            bands[place] = total[:, half * LEV : (half + 1) * LEV]
            sends.append(pltpu.make_async_copy(bands.at[place], out.at[place], osem.at[place]))
            sends[-1].start()

    for b in range(LAT // 4 + 1):
        far_cos = local[2 * EXT_X + b : 2 * EXT_X + b + 1, :]
        far_sin = local[2 * EXT_X + FAR + b : 2 * EXT_X + FAR + b + 1, :]
        near_cos, near_sin = local[0:EXT_X], local[EXT_X : 2 * EXT_X]
        cc, ss = far_cos * near_cos, far_sin * near_sin
        cs, sc = far_cos * near_sin, far_sin * near_cos
        put(b, cc + ss, cs - sc)
        if 0 < b < LAT // 4:
            put(LAT - b, cc - ss, cs + sc)
    for send in sends:
        send.wait()


def latitude_row(modes, tables):
    far = pl.BlockSpec(memory_space=pltpu.HBM)
    return pl.pallas_call(
        fourier_kernel,
        in_specs=[far, far],
        out_specs=far,
        out_shape=jax.ShapeDtypeStruct((LAT, EXT_X, LEV), jnp.bfloat16),
        scratch_shapes=[
            pltpu.VMEM((LATS * SLOTS, LEV), jnp.bfloat16),
            pltpu.VMEM((2 * EXT_X + 2 * FAR, COLUMNS), jnp.float32),
            pltpu.VMEM((LATS * SLOTS, LEV), jnp.float32),
            pltpu.VMEM((2 * COLUMNS, 2 * LEV), jnp.bfloat16),
            pltpu.VMEM((LAT, EXT_X, LEV), jnp.bfloat16),
            pltpu.SemaphoreType.DMA((2,)),
            pltpu.SemaphoreType.DMA((LAT,)),
        ],
    )(modes, tables)


def minmod(a, b):
    return jnp.maximum(jnp.minimum(a, b), jnp.minimum(jnp.maximum(a, b), 0.0))


def shifted(array, amount):
    return pltpu.roll(array, amount % array.shape[0], 0)


def flux(wind, gain, low, high, low_slope, high_slope):
    forward = wind > 0.0
    return wind * jnp.where(forward, low, high) + gain * jnp.where(forward, low_slope, high_slope)


def advect_kernel(
    where, tiles, ce, cn, ef, nf, west, east, wind_s, wind_n, out, qa, qb, us, gs
):
    band = where[0]
    qa[0:HALO] = tiles[HALO:, 1].astype(jnp.float32)
    qa[HALO : HALO + TILE_R] = tiles[:, 0].astype(jnp.float32)
    qa[HALO + TILE_R :] = tiles[:HALO, 1].astype(jnp.float32)
    qb[0:HALO] = jnp.zeros((HALO, EXT_X, LEV), jnp.float32)
    qb[HALO + TILE_R :] = jnp.zeros((HALO, EXT_X, LEV), jnp.float32)
    inner = slice(HALO, HALO + TILE_R)
    for d, (size, flag) in enumerate(((ce, ef), (cn, nf))):
        us[d, HALO - SOUTH_ROWS : HALO] = wind_s[d].astype(jnp.float32)
        us[d, HALO + TILE_R : HALO + TILE_R + NORTH_ROWS] = wind_n[d].astype(jnp.float32)
        us[d, inner, 0:HALO] = west[d].astype(jnp.float32)
        us[d, inner, HALO + TILE_X :] = east[d].astype(jnp.float32)
        us[d, inner, HALO : HALO + TILE_X] = jnp.where(flag[...] > 0, size[...], -size[...])

    def gains(r, carry):
        for d in range(2):
            speed = jnp.abs(us[d, r])
            gs[d, r] = 0.5 * speed * (1.0 - speed)
        return carry

    lax.fori_loop(HALO - SOUTH_ROWS, HALO + TILE_R + NORTH_ROWS, gains, 0)
    for t in range(1, STEPS + 1):
        old, new = (qa, qb) if t % 2 else (qb, qa)
        low = jnp.where(band == 0, HALO, 2 * t)
        high = jnp.where(band == WAVE - 1, HALO + TILE_R, EXT_R - 2 * t)

        def slope(r):
            here = old[r]
            return minmod(old[r + 1] - here, here - old[r - 1])

        def face(r, low_slope, high_slope):
            return flux(us[1, r], gs[1, r], old[r], old[r + 1], low_slope, high_slope)

        def row(r, carry):
            here_slope, below = carry
            here = old[r]
            next_slope = slope(r + 1)
            above = face(r, here_slope, next_slope)
            right = shifted(here, -1)
            jump = right - here
            steep = minmod(jump, shifted(jump, 1))
            east_face = flux(us[0, r], gs[0, r], here, right, steep, shifted(steep, -1))
            fresh = here - (east_face - shifted(east_face, 1)) - (above - below)
            if t == STEPS:
                out[r - HALO] = fresh[HALO : HALO + TILE_X]
            else:
                new[r] = fresh
            return next_slope, above

        first = slope(low)
        lax.fori_loop(low, high, row, (first, face(low - 1, slope(low - 1), first)))


def advected(band, tiles, winds, halos):
    return pl.pallas_call(
        advect_kernel,
        in_specs=[pl.BlockSpec(memory_space=pltpu.SMEM)]
        + [pl.BlockSpec(memory_space=pltpu.VMEM)] * 9,
        out_shape=jax.ShapeDtypeStruct((TILE_R, TILE_X, LEV), jnp.float32),
        scratch_shapes=[
            pltpu.VMEM((EXT_R, EXT_X, LEV), jnp.float32),
            pltpu.VMEM((EXT_R, EXT_X, LEV), jnp.float32),
            pltpu.VMEM((2, EXT_R, EXT_X, LEV), jnp.float32),
            pltpu.VMEM((2, EXT_R, EXT_X, LEV), jnp.float32),
        ],
        compiler_params=PARAMS,
    )(band[None], tiles, *winds, *halos)


def from_below(block, axis, wrap):
    pairs = [(i, (i + 1) % 16) for i in range(16 if wrap else 15)]
    return lax.ppermute(block, axis, pairs)


def from_above(block, axis, wrap):
    pairs = [((i + 1) % 16, i) for i in range(16 if wrap else 15)]
    return lax.ppermute(block, axis, pairs)


def per_device(
    control,
    vert_root,
    legendre,
    row_wavenumber,
    courant_east,
    courant_north,
    east_flags,
    north_flags,
):
    lat = lax.axis_index("lat").astype(jnp.int32)
    wave = lax.axis_index("wave").astype(jnp.int32)
    packed = packed_inputs(control, vert_root, legendre, row_wavenumber, lat * ORDERS)
    winds = jnp.stack(
        [
            jnp.where(flag > 0, size, -size).astype(jnp.bfloat16)
            for size, flag in ((courant_east, east_flags), (courant_north, north_flags))
        ]
    )
    west = from_below(winds[:, :, -HALO:], "lat", True)
    east = from_above(winds[:, :, :HALO], "lat", True)
    wide = jnp.concatenate([west, winds, east], axis=2)
    tables = angle_tables()
    packed = lax.all_to_all(packed, "wave", 0, 0, tiled=True)
    upper, lower = wide[:, -SOUTH_ROWS:], wide[:, :NORTH_ROWS]
    packed, upper, lower, tables = lax.optimization_barrier((packed, upper, lower, tables))
    modes = modes_of(packed)
    modes, upper, lower = lax.optimization_barrier((modes, upper, lower))
    wind_s = from_below(upper, "wave", False)
    wind_n = from_above(lower, "wave", False)
    modes = lax.all_to_all(modes.reshape(LATS, SLOTS, LEV), ("wave", "lat"), 0, 0, tiled=True)
    row = latitude_row(modes.reshape(LATS * SLOTS, LEV), tables)
    pairs = []
    for w in range(WAVE):
        for l in range(LAT):
            to = w - 1 if l < HALO else w + 1
            if 0 <= to < WAVE:
                pairs.append((w * LAT + l, to * LAT + l))
    next_row = lax.ppermute(row, ("wave", "lat"), pairs)
    rows = jnp.stack([row, next_row], axis=1)
    tiles = lax.all_to_all(rows, "lat", 0, 0, tiled=True)
    return advected(
        wave,
        tiles,
        (courant_east, courant_north, east_flags, north_flags),
        (west, east, wind_s, wind_n),
    )


def solution(mesh):
    return jax.shard_map(
        per_device,
        mesh=mesh,
        in_specs=(
            P("wave", "lat", None),
            P("wave", None, None),
            P("lat", "wave", None),
            P("wave"),
            P("wave", "lat", None),
            P("wave", "lat", None),
            P("wave", "lat", None),
            P("wave", "lat", None),
        ),
        out_specs=P("wave", "lat", None),
        check_vma=False,
    )
```

```python
import functools
import math

import jax
import jax.numpy as jnp
import numpy as np
from jax import lax
from jax.experimental import pallas as pl
from jax.experimental.pallas import tpu as pltpu
from jax.sharding import PartitionSpec as P

NW = 640
LEV = 128
STEPS = 4
NLON = 2 * NW
WAVE = 16
LAT = 16
ROWS = NW // WAVE
ORDERS = NW // LAT
LATS = 256
TILE_R = LATS // WAVE
TILE_X = NLON // LAT
HALO = 2 * STEPS
EXT_X = TILE_X + 2 * HALO
EXT_R = TILE_R + 2 * HALO
GROUP = 5
SLOTS = 8
ORDER_OF = ((0, 1, 2), (4, 3, 2))
SHARE = 24
SIZE_OF = (ROWS, ROWS, SHARE)
START_OF = (0, ROWS, 2 * ROWS)
PART_ROWS = 2 * ROWS + SHARE
CHUNK = 8
CHUNKS = ROWS // CHUNK
FAR = 8
COLUMNS = 3 * LATS
UNROLL = 2
EDGE = HALO - 1
PARAMS = pltpu.CompilerParams(vmem_limit_bytes=24 * 1024 * 1024)


def owned(w, slot):
    order = GROUP * (w // 2) + ORDER_OF[w % 2][slot]
    return order, ROWS - SHARE if slot == 2 and w % 2 else 0, SIZE_OF[slot]


def packing_kernel(
    wavenumber, first, control, vert, legendre, out, cbuf, vbuf, lbuf, scratch, whole, share, isem, osem
):
    loads = []
    for i in range(CHUNKS):
        rows = pl.ds(i * CHUNK * ORDERS, CHUNK * ORDERS)
        mats = pl.ds(i * CHUNK, CHUNK)
        loads.append(
            (
                pltpu.make_async_copy(legendre.at[mats], lbuf.at[mats], isem.at[2, i]),
                pltpu.make_async_copy(control.at[rows], cbuf.at[rows], isem.at[0, i]),
                pltpu.make_async_copy(vert.at[mats], vbuf.at[mats], isem.at[1, i]),
            )
        )
    for several in loads:
        for load in several[1:]:
            load.start()
    for several in loads:
        several[0].start()
    sends = []
    row_id = lax.broadcasted_iota(jnp.int32, (2 * LEV, 2 * LEV), 0)
    column = lax.broadcasted_iota(jnp.int32, (2 * LEV, 2 * LEV), 1)
    chosen = column == (row_id & 1) * LEV + (row_id >> 1)
    pick = jnp.where(chosen, 1.0, 0.0).astype(jnp.bfloat16)
    orders = first[0] + lax.broadcasted_iota(jnp.int32, (ORDERS, 2 * LEV), 0)
    for i in range(CHUNKS):
        for load in loads[i][1:]:
            load.wait()
        parts = jnp.dot(
            cbuf[i * CHUNK * ORDERS : (i + 1) * CHUNK * ORDERS],
            pick,
            preferred_element_type=jnp.float32,
        )
        for k in range(CHUNK):
            r = i * CHUNK + k
            rows = jnp.where(wavenumber[r] >= orders, parts[k * ORDERS : (k + 1) * ORDERS], 0.0)
            both = jnp.concatenate([rows[:, :LEV], rows[:, LEV:]], axis=0).astype(jnp.bfloat16)
            mixed = lax.dot_general(
                both, vbuf[r], (((1,), (1,)), ((), ())), preferred_element_type=jnp.float32
            )
            for p in range(2):
                scratch[p, pl.ds(r, ORDERS, stride=ROWS), :] = mixed[p * ORDERS : (p + 1) * ORDERS]
        loads[i][0].wait()
        for w in range(WAVE):
            for slot in range(3):
                order, start, size = owned(w, slot)
                if order // CHUNK == i:
                    send = pltpu.make_async_copy(
                        lbuf.at[order, pl.ds(start, size)],
                        out.at[w, pl.ds(PART_ROWS + START_OF[slot], size)],
                        osem.at[0, w, slot],
                    )
                    send.start()
                    sends.append(send)
    for w in range(WAVE):
        for slot in range(3):
            order, start, size = owned(w, slot)
            base = order * ROWS + start
            values = jnp.concatenate(
                [scratch[0, base : base + size], scratch[1, base : base + size]], axis=1
            )
            if slot < 2:
                kept = whole.at[w, slot]
            else:
                kept = share.at[w]
                if w % 2:
                    own = lax.broadcasted_iota(jnp.int32, values.shape, 0) >= 2 * SHARE - ROWS
                    values = jnp.where(own, values, 0.0)
            kept[...] = values.astype(jnp.bfloat16)
            sends.append(
                pltpu.make_async_copy(
                    kept, out.at[w, pl.ds(START_OF[slot], size)], osem.at[1, w, slot]
                )
            )
            sends[-1].start()
    for send in sends:
        send.wait()


def packed_inputs(control, vert_root, legendre, row_wavenumber, first_order):
    smem = pl.BlockSpec(memory_space=pltpu.SMEM)
    far = pl.BlockSpec(memory_space=pltpu.HBM)
    return pl.pallas_call(
        packing_kernel,
        in_specs=[smem, smem, far, far, far],
        out_specs=far,
        out_shape=jax.ShapeDtypeStruct((WAVE, 2 * PART_ROWS, 2 * LEV), jnp.bfloat16),
        scratch_shapes=[
            pltpu.VMEM((ROWS * ORDERS, 2 * LEV), jnp.bfloat16),
            pltpu.VMEM((ROWS, LEV, LEV), jnp.bfloat16),
            pltpu.VMEM((ORDERS, ROWS, LATS), jnp.bfloat16),
            pltpu.VMEM((2, ORDERS * ROWS, LEV), jnp.float32),
            pltpu.VMEM((WAVE, 2, ROWS, 2 * LEV), jnp.bfloat16),
            pltpu.VMEM((WAVE, SHARE, 2 * LEV), jnp.bfloat16),
            pltpu.SemaphoreType.DMA((3, CHUNKS)),
            pltpu.SemaphoreType.DMA((2, WAVE, 3)),
        ],
    )(
        row_wavenumber,
        first_order[None],
        control.reshape(ROWS * ORDERS, 2 * LEV),
        vert_root,
        legendre,
    )


def modes_kernel(packed, out, left, right, result):
    result[...] = jnp.zeros(result.shape, jnp.float32)
    for slot in range(3):
        size = SIZE_OF[slot]
        for s in range(WAVE):
            rows = slice(s * size, (s + 1) * size)
            for start, side in ((START_OF[slot], right), (PART_ROWS + START_OF[slot], left)):
                block = packed[s, start // 8 : (start + size) // 8].astype(jnp.float32)
                side[rows, :] = block.reshape(size, 2 * LEV)
        total = lax.dot_general(
            left[0 : WAVE * size].astype(jnp.bfloat16),
            right[0 : WAVE * size].astype(jnp.bfloat16),
            (((0,), (0,)), ((), ())),
            preferred_element_type=jnp.float32,
        )
        for p in range(2):
            result[pl.ds(2 * slot + p, LATS, stride=SLOTS), :] = total[:, p * LEV : (p + 1) * LEV]
    out[...] = result[...].astype(jnp.bfloat16)


def modes_of(packed):
    return pl.pallas_call(
        modes_kernel,
        out_shape=jax.ShapeDtypeStruct((LATS * SLOTS, LEV), jnp.bfloat16),
        scratch_shapes=[
            pltpu.VMEM((NW, LATS), jnp.float32),
            pltpu.VMEM((NW, 2 * LEV), jnp.float32),
            pltpu.VMEM((LATS * SLOTS, LEV), jnp.float32),
        ],
        compiler_params=PARAMS,
    )(packed.reshape(WAVE, PART_ROWS // 4, 8, 2 * LEV))


def angle_tables():
    order = np.zeros((3, WAVE, LAT), np.int32)
    for w in range(WAVE):
        for slot in range(3):
            order[slot, w] = np.arange(LAT) * ORDERS + owned(w, slot)[0]
    order = jnp.asarray(order.reshape(-1))
    weight = jnp.where(order == 0, 1.0, 2.0).astype(jnp.float32) * (1.0 / math.sqrt(NLON))

    def turn(steps):
        return (steps % NLON).astype(jnp.float32) * (2.0 * math.pi / NLON)

    local = jnp.arange(EXT_X, dtype=jnp.int32) - HALO + NLON
    near = turn(order[None, :] * local[:, None])
    far = turn(order[None, :] * (TILE_X * jnp.arange(FAR, dtype=jnp.int32))[:, None])
    return jnp.concatenate(
        [weight * jnp.cos(near), -weight * jnp.sin(near), jnp.cos(far), jnp.sin(far)]
    )


def fourier_kernel(modes, tables, out, held, local, wide, rhs, bands, isem, osem):
    load_modes = pltpu.make_async_copy(modes, held, isem.at[0])
    load_tables = pltpu.make_async_copy(tables, local, isem.at[1])
    load_modes.start()
    load_tables.start()
    load_modes.wait()
    wide[...] = held[...].astype(jnp.float32)
    group = lax.broadcasted_iota(jnp.int32, (LATS, LEV), 0) // (2 * LAT)
    for slot in range(3):
        even = (group + ORDER_OF[0][slot]) % 2 == 0
        for p in range(2):
            rows = wide[pl.ds(2 * slot + p, LATS, stride=SLOTS), :]
            start = p * COLUMNS + slot * LATS
            rhs[start : start + LATS, :LEV] = rows.astype(jnp.bfloat16)
            rhs[start : start + LATS, LEV:] = jnp.where(even, rows, -rows).astype(jnp.bfloat16)
    load_tables.wait()
    sends = []

    def put(band, real, imaginary):
        basis = jnp.concatenate(
            [real.astype(jnp.bfloat16), imaginary.astype(jnp.bfloat16)], axis=1
        )
        total = jnp.dot(basis, rhs[...], preferred_element_type=jnp.float32).astype(jnp.bfloat16)
        for half in range(2):
            place = (band + half * (LAT // 2)) % LAT
            bands[place] = total[:, half * LEV : (half + 1) * LEV]
            sends.append(pltpu.make_async_copy(bands.at[place], out.at[place], osem.at[place]))
            sends[-1].start()

    for b in range(LAT // 4 + 1):
        far_cos = local[2 * EXT_X + b : 2 * EXT_X + b + 1, :]
        far_sin = local[2 * EXT_X + FAR + b : 2 * EXT_X + FAR + b + 1, :]
        near_cos, near_sin = local[0:EXT_X], local[EXT_X : 2 * EXT_X]
        cc, ss = far_cos * near_cos, far_sin * near_sin
        cs, sc = far_cos * near_sin, far_sin * near_cos
        put(b, cc + ss, cs - sc)
        if 0 < b < LAT // 4:
            put(LAT - b, cc - ss, cs + sc)
    for send in sends:
        send.wait()


def latitude_row(modes, tables):
    far = pl.BlockSpec(memory_space=pltpu.HBM)
    return pl.pallas_call(
        fourier_kernel,
        in_specs=[far, far],
        out_specs=far,
        out_shape=jax.ShapeDtypeStruct((LAT, EXT_X, LEV), jnp.bfloat16),
        scratch_shapes=[
            pltpu.VMEM((LATS * SLOTS, LEV), jnp.bfloat16),
            pltpu.VMEM((2 * EXT_X + 2 * FAR, COLUMNS), jnp.float32),
            pltpu.VMEM((LATS * SLOTS, LEV), jnp.float32),
            pltpu.VMEM((2 * COLUMNS, 2 * LEV), jnp.bfloat16),
            pltpu.VMEM((LAT, EXT_X, LEV), jnp.bfloat16),
            pltpu.SemaphoreType.DMA((2,)),
            pltpu.SemaphoreType.DMA((LAT,)),
        ],
    )(modes, tables)


def minmod(a, b):
    return jnp.maximum(jnp.minimum(a, b), jnp.minimum(jnp.maximum(a, b), 0.0))


def shifted(array, amount):
    return pltpu.roll(array, amount % array.shape[0], 0)


def flux(wind, gain, low, high, low_slope, high_slope):
    forward = wind > 0.0
    return wind * jnp.where(forward, low, high) + gain * jnp.where(forward, low_slope, high_slope)


def advect_kernel(
    where, middle, halo, ce, cn, ef, nf, west, east, early, late, out, qa, qb, us, gs
):
    band = where[0]
    odd = band % 2 == 1
    qa[0:HALO] = halo[HALO:].astype(jnp.float32)
    qa[HALO : HALO + TILE_R] = middle[...].astype(jnp.float32)
    qa[HALO + TILE_R :] = halo[:HALO].astype(jnp.float32)
    qb[0:HALO] = jnp.zeros((HALO, EXT_X, LEV), jnp.float32)
    qb[HALO + TILE_R :] = jnp.zeros((HALO, EXT_X, LEV), jnp.float32)
    inner = slice(HALO, HALO + TILE_R)
    for d, (size, flag) in enumerate(((ce, ef), (cn, nf))):
        first, second = early[d].astype(jnp.float32), late[d].astype(jnp.float32)
        us[d, HALO - EDGE : HALO] = jnp.where(odd, first, second)
        us[d, HALO + TILE_R : HALO + TILE_R + EDGE] = jnp.where(odd, second, first)
        us[d, inner, 0:HALO] = west[d].astype(jnp.float32)
        us[d, inner, HALO + TILE_X :] = east[d].astype(jnp.float32)
        us[d, inner, HALO : HALO + TILE_X] = jnp.where(flag[...] > 0, size[...], -size[...])

    def gains(r, carry):
        for d in range(2):
            speed = jnp.abs(us[d, r])
            gs[d, r] = 0.5 * speed * (1.0 - speed)
        return carry

    lax.fori_loop(HALO - EDGE, HALO + TILE_R + EDGE, gains, 0)
    keep = jnp.where(band == WAVE - 1, 0.0, 1.0)
    for t in range(1, STEPS + 1):
        old, new = (qa, qb) if t % 2 else (qb, qa)

        def rows(i, carry, start):
            slope, below = carry
            first = start + UNROLL * i
            here, above = old[first], old[first + 1]
            jump = above - here
            for k in range(UNROLL):
                r = first + k
                beyond = old[r + 2]
                next_jump = beyond - above
                next_slope = minmod(next_jump, jump)
                top = flux(us[1, r], gs[1, r], here, above, slope, next_slope)
                right = shifted(here, -1)
                step = right - here
                steep = minmod(step, shifted(step, 1))
                east_face = flux(us[0, r], gs[0, r], here, right, steep, shifted(steep, -1))
                fresh = here - (east_face - shifted(east_face, 1)) - (top - below)
                if t == STEPS:
                    out[r - HALO] = fresh[HALO : HALO + TILE_X]
                else:
                    new[r] = fresh
                here, above, jump, slope, below = above, beyond, next_jump, next_slope, top
            return slope, below

        low, top_row, high = 2 * t, HALO + TILE_R, EXT_R - 2 * t
        far, down, here, up = (old[low + d] for d in (-2, -1, 0, 1))
        slope = minmod(up - here, here - down)
        face = flux(us[1, low - 1], gs[1, low - 1], down, here, minmod(here - down, down - far), slope)
        carry = lax.fori_loop(
            0, (top_row - low) // UNROLL, functools.partial(rows, start=low), (slope, face)
        )
        if high > top_row:
            carry = (carry[0], carry[1] * keep)
            lax.fori_loop(0, (high - top_row) // UNROLL, functools.partial(rows, start=top_row), carry)


def advected(band, middle, halo, winds, halos):
    return pl.pallas_call(
        advect_kernel,
        in_specs=[pl.BlockSpec(memory_space=pltpu.SMEM)]
        + [pl.BlockSpec(memory_space=pltpu.VMEM)] * 10,
        out_shape=jax.ShapeDtypeStruct((TILE_R, TILE_X, LEV), jnp.float32),
        scratch_shapes=[
            pltpu.VMEM((EXT_R, EXT_X, LEV), jnp.float32),
            pltpu.VMEM((EXT_R, EXT_X, LEV), jnp.float32),
            pltpu.VMEM((2, EXT_R, EXT_X, LEV), jnp.float32),
            pltpu.VMEM((2, EXT_R, EXT_X, LEV), jnp.float32),
        ],
        compiler_params=PARAMS,
    )(band[None], middle, halo, *winds, *halos)


def from_below(block, axis, wrap):
    pairs = [(i, (i + 1) % 16) for i in range(16 if wrap else 15)]
    return lax.ppermute(block, axis, pairs)


def from_above(block, axis, wrap):
    pairs = [((i + 1) % 16, i) for i in range(16 if wrap else 15)]
    return lax.ppermute(block, axis, pairs)


def per_device(
    control,
    vert_root,
    legendre,
    row_wavenumber,
    courant_east,
    courant_north,
    east_flags,
    north_flags,
):
    lat = lax.axis_index("lat").astype(jnp.int32)
    wave = lax.axis_index("wave").astype(jnp.int32)
    packed = packed_inputs(control, vert_root, legendre, row_wavenumber, lat * ORDERS)
    winds = jnp.stack(
        [
            jnp.where(flag > 0, size, -size).astype(jnp.bfloat16)
            for size, flag in ((courant_east, east_flags), (courant_north, north_flags))
        ]
    )
    west = from_below(winds[:, :, -HALO:], "lat", True)
    east = from_above(winds[:, :, :HALO], "lat", True)
    wide = jnp.concatenate([west, winds, east], axis=2)
    tables = angle_tables()
    packed = lax.all_to_all(packed, "wave", 0, 0, tiled=True)
    odd = wave % 2 == 1
    upper, lower = wide[:, -EDGE:], wide[:, :EDGE]
    early = lax.ppermute(jnp.where(odd, lower, upper), "wave", [(w, w ^ 1) for w in range(WAVE)])
    late = jnp.where(odd, upper, lower)
    packed, early, late, tables = lax.optimization_barrier((packed, early, late, tables))
    modes = modes_of(packed)
    modes, late = lax.optimization_barrier((modes, late))
    ends = [(w, w + 1) for w in range(1, WAVE - 1, 2)]
    late = lax.ppermute(late, "wave", ends + [(j, i) for i, j in ends])
    modes = lax.all_to_all(modes.reshape(LATS, SLOTS, LEV), ("wave", "lat"), 0, 0, tiled=True)
    row = latitude_row(modes.reshape(LATS * SLOTS, LEV), tables)
    pairs = []
    for w in range(WAVE):
        for l in range(LAT):
            to = w - 1 if l < HALO else w + 1
            if 0 <= to < WAVE:
                pairs.append((w * LAT + l, to * LAT + l))
    next_row = lax.ppermute(row, ("wave", "lat"), pairs)
    middle = lax.all_to_all(row, "lat", 0, 0, tiled=True)
    halo = lax.all_to_all(next_row, "lat", 0, 0, tiled=True)
    return advected(
        wave,
        middle,
        halo,
        (courant_east, courant_north, east_flags, north_flags),
        (west, east, early, late),
    )


def solution(mesh):
    return jax.shard_map(
        per_device,
        mesh=mesh,
        in_specs=(
            P("wave", "lat", None),
            P("wave", None, None),
            P("lat", "wave", None),
            P("wave"),
            P("wave", "lat", None),
            P("wave", "lat", None),
            P("wave", "lat", None),
            P("wave", "lat", None),
        ),
        out_specs=P("wave", "lat", None),
        check_vma=False,
    )
```
